32 devices in a mesh: side: 4 (over z), rep: 8 (over y, x, core).
Axes of the slice: x: 2, y: 2, z: 4, core: 2. Of those that a mesh axis runs over, the one named last changes fastest.
Arguments:
- w_up: float32 [4, 1, 2048, 2816], P('side', None, 'rep')
- w_down: float32 [4, 1, 2816, 2048], P('side', None, None, 'rep')
- g_up: float32 [4, 1, 2048, 2816], P('side', None, 'rep')
- g_down: float32 [4, 1, 2816, 2048], P('side', None, None, 'rep')
- learn_rate: float32 [1], replicated
- old_up: bfloat16 [4, 8, 1, 2048, 2816], P('side', 'rep')
- old_down: bfloat16 [4, 8, 1, 2816, 2048], P('side', 'rep')
- prompts: bfloat16 [4, 8, 1024, 2048], P('side', 'rep')
Outputs:
- output 1: float32 [4, 1, 2048, 2816], P('side', None, 'rep')
- output 2: float32 [4, 1, 2816, 2048], P('side', None, None, 'rep')
- output 3: bfloat16 [4, 8, 1024, 2048], P('side', 'rep')
All inputs are finite; a program needn't handle non-finite values.
Results may differ from the reference program's by a relative error of at most 0.00721101.
Values are sent between devices in bfloat16 or wider.
A program may use at most 1 GiB of HBM per device.

```python
import jax
import jax.numpy as jnp
from jax import lax

MODEL_DIM = 2048
HIDDEN_DIM = 5632
LAYERS = 1
TOKENS = 1024
REPLICAS = 8
TP_WIDTH = 2
SHARD_DIM = HIDDEN_DIM // TP_WIDTH


def split_up(full):
    return jnp.transpose(full.reshape(LAYERS, MODEL_DIM, TP_WIDTH, SHARD_DIM), (2, 0, 1, 3))


def split_down(full):
    return jnp.transpose(full.reshape(LAYERS, TP_WIDTH, SHARD_DIM, MODEL_DIM), (1, 0, 2, 3))


def merge_up(blocks):
    return jnp.transpose(blocks, (1, 2, 0, 3)).reshape(LAYERS, MODEL_DIM, HIDDEN_DIM)


def merge_down(blocks):
    return jnp.transpose(blocks, (1, 0, 2, 3)).reshape(LAYERS, HIDDEN_DIM, MODEL_DIM)


def trainer_slots(blocks):
    return jnp.concatenate([blocks, jnp.zeros_like(blocks)], axis=0)


def generator_slots(blocks):
    copies = jnp.broadcast_to(blocks[:, None], (TP_WIDTH, REPLICAS) + blocks.shape[1:])
    return jnp.concatenate([jnp.zeros_like(copies), copies], axis=0)


def setup_inputs(seed: int = 0) -> dict:
    rng_keys = jax.random.split(jax.random.key(seed), 8)
    up_scale = MODEL_DIM ** -0.5
    down_scale = HIDDEN_DIM ** -0.5
    up_shape = (LAYERS, MODEL_DIM, HIDDEN_DIM)
    down_shape = (LAYERS, HIDDEN_DIM, MODEL_DIM)
    w_up_full = jax.random.normal(rng_keys[0], up_shape, jnp.float32) * up_scale
    w_down_full = jax.random.normal(rng_keys[1], down_shape, jnp.float32) * down_scale
    g_up_full = jax.random.normal(rng_keys[2], up_shape, jnp.float32) * up_scale
    g_down_full = jax.random.normal(rng_keys[3], down_shape, jnp.float32) * down_scale
    learn_rate = jax.random.uniform(rng_keys[4], (1,), jnp.float32, minval=0.15, maxval=0.3)
    stale_up = (w_up_full + 0.2 * up_scale * jax.random.normal(rng_keys[5], up_shape, jnp.float32)).astype(jnp.bfloat16)
    stale_down = (w_down_full + 0.2 * down_scale * jax.random.normal(rng_keys[6], down_shape, jnp.float32)).astype(jnp.bfloat16)
    prompt_rows = jax.random.normal(rng_keys[7], (REPLICAS, TOKENS, MODEL_DIM), jnp.float32).astype(jnp.bfloat16)
    prompt_copies = jnp.broadcast_to(prompt_rows[None], (TP_WIDTH,) + prompt_rows.shape)
    return {
        "w_up": trainer_slots(split_up(w_up_full)),
        "w_down": trainer_slots(split_down(w_down_full)),
        "g_up": trainer_slots(split_up(g_up_full)),
        "g_down": trainer_slots(split_down(g_down_full)),
        "learn_rate": learn_rate,
        "old_up": generator_slots(split_up(stale_up)),
        "old_down": generator_slots(split_down(stale_down)),
        "prompts": jnp.concatenate([jnp.zeros_like(prompt_copies), prompt_copies], axis=0),
    }


def layer_step(hidden, weights):
    up_mat, down_mat = weights
    pre_act = jnp.dot(hidden, up_mat, preferred_element_type=jnp.float32)
    act_val = jax.nn.gelu(pre_act, approximate=False).astype(jnp.bfloat16)
    branch = jnp.dot(act_val, down_mat, preferred_element_type=jnp.float32)
    return (hidden.astype(jnp.float32) + branch).astype(jnp.bfloat16), None


def reference(w_up, w_down, g_up, g_down, learn_rate, old_up, old_down, prompts):
    step_rate = learn_rate[0]
    new_up = w_up - step_rate * g_up
    new_down = w_down - step_rate * g_down
    delta_up = merge_up((new_up - w_up)[:TP_WIDTH].astype(jnp.bfloat16)).astype(jnp.float32)
    delta_down = merge_down((new_down - w_down)[:TP_WIDTH].astype(jnp.bfloat16)).astype(jnp.float32)
    stale_gen_up = jnp.swapaxes(old_up[TP_WIDTH:], 0, 1)
    stale_gen_down = jnp.swapaxes(old_down[TP_WIDTH:], 0, 1)

    def one_replica(operands):
        rep_up, rep_down, rep_x = operands
        gen_up = (merge_up(rep_up).astype(jnp.float32) + delta_up).astype(jnp.bfloat16)
        gen_down = (merge_down(rep_down).astype(jnp.float32) + delta_down).astype(jnp.bfloat16)
        final_h, _ = lax.scan(layer_step, rep_x, (gen_up, gen_down))
        return final_h

    gen_out = lax.map(one_replica, (stale_gen_up, stale_gen_down, prompts[TP_WIDTH]))
    gen_copies = jnp.broadcast_to(gen_out[None], (TP_WIDTH,) + gen_out.shape)
    outputs = jnp.concatenate([jnp.zeros_like(gen_copies), gen_copies], axis=0)
    return new_up, new_down, outputs
```

```python
import functools

import jax
import jax.numpy as jnp
from jax import lax
from jax.experimental import pallas as pl
from jax.experimental.pallas import tpu as pltpu
from jax.sharding import PartitionSpec as P

MESH = pl.DeviceIdType.MESH
F32 = jnp.float32
BF16 = jnp.bfloat16
DX, DY, DZ = 1, 2, 4
STAGES = 4


def exact_gelu(v):
    return (0.5 * v) * (1.0 + lax.erf(v * (0.5**0.5)))


def sync_kernel(
    n_chunks, width, rows, up_delta, down_delta, old_up, old_down, prompts, y_ref,
    weights, acc, hidden, stale,
    up_recv, down_recv, send_sem, recv_sem, pair_recv, stale_sem, io_sem, pace_sem,
):
    side = lax.axis_index("side")
    rep = lax.axis_index("rep")
    core = rep % 2
    xpos = (rep // 2) % 2
    ypos = rep // 4
    is_gen = side >= 2
    rank = side % 2
    tokens = hidden.shape[0]

    barrier = pltpu.get_barrier_semaphore()

    def ping(sem, to_side, to_rep):
        pl.semaphore_signal(sem, inc=1, device_id=(to_side, to_rep), device_id_type=MESH)

    x_rep = rep + 2 * (1 - 2 * xpos)
    y_rep = rep + 4 * (1 - 2 * ypos)
    pair_rep = rep + (1 - 2 * core)
    z_side = 5 - side

    def columns(c):
        return pl.ds(pl.multiple_of(c * width, width), width)

    mine = pl.ds(pl.multiple_of(rep * rows, rows), rows)

    def delta_copies(c, to_side):
        slot = weights.at[c, rank, rep // 2, core]
        up = pltpu.make_async_remote_copy(
            src_ref=up_delta.at[:, columns(c)], dst_ref=slot.at[0], send_sem=send_sem.at[c, 0],
            recv_sem=up_recv.at[c], device_id=(to_side, rep), device_id_type=MESH,
        )
        down = pltpu.make_async_remote_copy(
            src_ref=down_delta.at[columns(c), :], dst_ref=slot.at[1], send_sem=send_sem.at[c, 1],
            recv_sem=down_recv.at[c], device_id=(to_side, rep), device_id_type=MESH,
        )
        return up, down

    def prompts_in():
        return pltpu.make_async_copy(prompts.at[0, 0], hidden, io_sem.at[0])

    def result_out():
        return pltpu.make_async_copy(hidden, y_ref.at[0, 0], io_sem.at[1])

    @pl.when(side < 2)
    def _():
        prompts_in().start()
        ping(barrier, side + 2, rep)
        ping(barrier, 1 - side, rep)
        pl.semaphore_wait(barrier, 2)

        def send(c, carry):
            @pl.when((side == 0) & (c >= 1))
            def _():
                pl.semaphore_wait(pace_sem, 1)

            for copy in delta_copies(c, side + 2):
                copy.start()

            @pl.when((side == 1) & (c >= 1))
            def _():
                for copy in delta_copies(c - 1, side + 2):
                    copy.wait_send()
                ping(pace_sem, 0, rep)

            return carry

        lax.fori_loop(0, n_chunks, send, 0)

        @pl.when(side == 1)
        def _():
            for copy in delta_copies(n_chunks - 1, side + 2):
                copy.wait_send()

        @pl.when(side == 0)
        def _():
            def drain(c, carry):
                for copy in delta_copies(c, side + 2):
                    copy.wait_send()
                return carry

            lax.fori_loop(0, n_chunks, drain, 0)

        prompts_in().wait()
        result_out().start()
        result_out().wait()

    @pl.when(is_gen)
    def _():
        prompts_in().start()

        def slot_at(d):
            t = 1 - rank if d & DZ else rank
            yy = 1 - ypos if d & DY else ypos
            xx = 1 - xpos if d & DX else xpos
            return t, yy * 2 + xx

        def stale_copies(c):
            up = pltpu.make_async_copy(
                old_up.at[0, 0, 0, mine, columns(c)], stale.at[c % 2, 0], stale_sem.at[c % 2, 0]
            )
            down = pltpu.make_async_copy(
                old_down.at[0, 0, 0, columns(c), mine], stale.at[c % 2, 1], stale_sem.at[c % 2, 1]
            )
            return up, down

        def message(c, d, axis, send_slot):
            t, yx = slot_at(d)
            ref = weights.at[c, t, yx, core]
            if axis == DX:
                to = (side, x_rep)
            elif axis == DY:
                to = (side, y_rep)
            else:
                to = (z_side, rep)
            return pltpu.make_async_remote_copy(
                src_ref=ref, dst_ref=ref, send_sem=send_sem.at[c, send_slot], recv_sem=recv_sem.at[c, d | axis],
                device_id=to, device_id_type=MESH,
            )

        def arrival(c, d):
            t, yx = slot_at(d)
            ref = weights.at[c, t, yx, core]
            return pltpu.make_async_remote_copy(
                src_ref=ref, dst_ref=ref, send_sem=send_sem.at[c, 0], recv_sem=recv_sem.at[c, d],
                device_id=(side, rep), device_id_type=MESH,
            )

        def pair_message(c, dz):
            t = 1 - rank if dz else rank
            ref = weights.at[c, t, :, core]
            return pltpu.make_async_remote_copy(
                src_ref=ref, dst_ref=ref, send_sem=send_sem.at[c, 7 + dz], recv_sem=pair_recv.at[c, dz],
                device_id=(side, pair_rep), device_id_type=MESH,
            )

        def pair_arrival(c, dz):
            t = 1 - rank if dz else rank
            ref = weights.at[c, t, :, 1 - core]
            return pltpu.make_async_remote_copy(
                src_ref=ref, dst_ref=ref, send_sem=send_sem.at[c, 0], recv_sem=pair_recv.at[c, dz],
                device_id=(side, pair_rep), device_id_type=MESH,
            )

        for c in (0, 1):
            for copy in stale_copies(c):
                copy.start()
        ping(barrier, side, x_rep)
        ping(barrier, side, y_rep)
        ping(barrier, side, pair_rep)
        ping(barrier, z_side, rep)
        ping(barrier, side - 2, rep)

        def clear(i, carry):
            acc[pl.ds(pl.multiple_of(i * 64, 64), 64), :] = jnp.zeros((64, acc.shape[1]), F32)
            return carry

        lax.fori_loop(0, tokens // 64, clear, 0)
        pl.semaphore_wait(barrier, 5)
        prompts_in().wait()

        def odd(c):
            return c % 2 == 1

        def via_x(c):
            return c % 5 == 1

        def via_y(c):
            return c % 5 == 4

        def via_z(c):
            return (c % 5 != 1) & (c % 5 != 4)

        hop1 = ((0, DX, 0, None), (0, DY, 1, None), (0, DZ, 2, None))
        hop2 = (
            (DZ, DX, 3, None),
            (DZ, DY, 4, None),
            (DY, DX, 5, lambda c: c % 2 == 0),
            (DX, DY, 5, odd),
        )
        hop3 = ((DY | DZ, DX, 6, via_x), (DX | DZ, DY, 6, via_y), (DX | DY, DZ, 6, via_z))

        def send_all(c, routes):
            for d, axis, send_slot, which in routes:
                if which is None:
                    message(c, d, axis, send_slot).start()
                else:

                    @pl.when(which(c))
                    def _(d=d, axis=axis, send_slot=send_slot):
                        message(c, d, axis, send_slot).start()

        def own_chunk(c):
            slot = weights.at[c, rank, rep // 2, core]
            for half, sem in ((0, up_recv), (1, down_recv)):
                pltpu.make_async_remote_copy(
                    src_ref=slot.at[half], dst_ref=slot.at[half], send_sem=send_sem.at[c, 0], recv_sem=sem.at[c],
                    device_id=(side - 2, rep), device_id_type=MESH,
                ).wait_recv()
            for copy in stale_copies(c):
                copy.wait()
            for half in (0, 1):
                slot[half] = (stale[c % 2, half].astype(F32) + slot[half].astype(F32)).astype(BF16)

            @pl.when(c + 2 < n_chunks)
            def _():
                for copy in stale_copies(c + 2):
                    copy.start()

        block = min(512, tokens)

        def multiply(c, t):
            def body(m, carry):
                here = pl.ds(pl.multiple_of(m * block, block), block)
                up_mat = weights[c, t, :, :, 0].reshape(8 * rows, width)
                pre_act = jnp.dot(hidden[here, :], up_mat, preferred_element_type=F32)
                act = exact_gelu(pre_act).astype(BF16)
                for piece in range(8):
                    cols = slice(piece * rows, (piece + 1) * rows)
                    acc[here, cols] += jnp.dot(
                        act, weights[c, t, piece // 2, piece % 2, 1], preferred_element_type=F32
                    )
                return carry

            lax.fori_loop(0, tokens // block, body, 0)

        def step(i, carry):
            @pl.when(i < n_chunks)
            def _():
                own_chunk(i)

            @pl.when((i >= 1) & (i < n_chunks + 1))
            def _():
                for d in (DX, DY, DZ):
                    arrival(i - 1, d).wait_recv()
                send_all(i - 1, hop2)

            @pl.when(i < n_chunks)
            def _():
                send_all(i, hop1)

            @pl.when((i >= 2) & (i < n_chunks + 2))
            def _():
                for d in (DX | DY, DX | DZ, DY | DZ):
                    arrival(i - 2, d).wait_recv()
                send_all(i - 2, hop3)
                pair_message(i - 2, 0).start()

            @pl.when((i >= 3) & (i < n_chunks + 3))
            def _():
                arrival(i - 3, DX | DY | DZ).wait_recv()
                pair_message(i - 3, 1).start()

            @pl.when(i >= STAGES)
            def _():
                c = i - STAGES
                for dz in (0, 1):
                    pair_arrival(c, dz).wait_recv()

                def ranks(t, carry):
                    multiply(c, t)
                    return carry

                lax.fori_loop(0, 2, ranks, 0)

            return carry

        lax.fori_loop(0, n_chunks + STAGES, step, 0)

        def finish(m, carry):
            here = pl.ds(pl.multiple_of(m * 64, 64), 64)
            hidden[here, :] = (hidden[here, :].astype(F32) + acc[here, :]).astype(BF16)
            return carry

        lax.fori_loop(0, tokens // 64, finish, 0)
        result_out().start()

        def drain(c, carry):
            for d, axis, send_slot, _ in hop1 + hop2[:3] + hop3[:1]:
                message(c, d, axis, send_slot).wait_send()
            for dz in (0, 1):
                pair_message(c, dz).wait_send()
            return carry

        lax.fori_loop(0, n_chunks, drain, 0)
        result_out().wait()


def solution(mesh):
    up_spec = P("side", None, "rep", None)
    down_spec = P("side", None, None, "rep")
    copy_spec = P("side", "rep", None, None, None)
    token_spec = P("side", "rep", None, None)

    def local_step(w_up, w_down, g_up, g_down, learn_rate, old_up, old_down, prompts):
        step_rate = learn_rate[0]
        new_up = w_up - step_rate * g_up
        new_down = w_down - step_rate * g_down
        delta_up = (new_up - w_up)[0, 0].astype(BF16)
        delta_down = (new_down - w_down)[0, 0].astype(BF16)
        rows, shard = delta_up.shape
        width = 256 if shard % 256 == 0 else 128
        n_chunks = shard // width
        tokens, model = prompts.shape[2:]
        y = pl.pallas_call(
            functools.partial(sync_kernel, n_chunks, width, rows),
            out_shape=jax.ShapeDtypeStruct(prompts.shape, BF16),
            in_specs=[pl.BlockSpec(memory_space=pl.ANY)] * 5,
            out_specs=pl.BlockSpec(memory_space=pl.ANY),
            scratch_shapes=[
                pltpu.VMEM((n_chunks, 2, 4, 2, 2, rows, width), BF16),
                pltpu.VMEM((tokens, model), F32),
                pltpu.VMEM((tokens, model), BF16),
                pltpu.VMEM((2, 2, rows, width), BF16),
                pltpu.SemaphoreType.DMA((n_chunks,)),
                pltpu.SemaphoreType.DMA((n_chunks,)),
                pltpu.SemaphoreType.DMA((n_chunks, 9)),
                pltpu.SemaphoreType.DMA((n_chunks, 8)),
                pltpu.SemaphoreType.DMA((n_chunks, 2)),
                pltpu.SemaphoreType.DMA((2, 2)),
                pltpu.SemaphoreType.DMA((2,)),
                pltpu.SemaphoreType.REGULAR,
            ],
            compiler_params=pltpu.CompilerParams(
                collective_id=0, has_side_effects=True, vmem_limit_bytes=67043328
            ),
        )(delta_up, delta_down, old_up, old_down, prompts)
        return new_up, new_down, y

    return jax.shard_map(
        local_step,
        mesh=mesh,
        in_specs=(up_spec, down_spec, up_spec, down_spec, P(None), copy_spec, copy_spec, token_spec),
        out_specs=(up_spec, down_spec, token_spec),
        check_vma=False,
    )
```

```python
import functools

import jax
import jax.numpy as jnp
from jax import lax
from jax.experimental import pallas as pl
from jax.experimental.pallas import tpu as pltpu
from jax.sharding import PartitionSpec as P

MESH = pl.DeviceIdType.MESH
F32 = jnp.float32
BF16 = jnp.bfloat16
LANES = 128
DX, DY, DZ = 1, 2, 4
WHOLE, UPPER, LOWER = (0, 4), (0, 2), (2, 4)
ARRIVALS = {
    (DX, WHOLE): 0, (DY, WHOLE): 1, (DZ, WHOLE): 2, (DX | DZ, WHOLE): 3, (DY | DZ, WHOLE): 4,
    (DX | DY, UPPER): 5, (DX | DY, LOWER): 6, (DX | DY | DZ, WHOLE): 7,
}
HOP1 = ((0, DZ, WHOLE), (0, DX, WHOLE), (0, DY, WHOLE))
HOP2 = ((DZ, DX, WHOLE), (DZ, DY, WHOLE), (DY, DX, UPPER), (DX, DY, LOWER))
HOP3 = ((DX | DY, DZ, WHOLE),)
SENDS = HOP1 + HOP2 + HOP3
N_SEMS = len(SENDS) + 2
WINDOW = 6
PACE = 2
LAST = 4


def exact_gelu(v):
    return (0.5 * v) * (1.0 + lax.erf(v * (0.5**0.5)))


def sync_kernel(
    n_chunks, up_delta, down_delta, old_up, old_down, prompts, y_ref,
    weights, acc, hidden, stale,
    own_recv, send_sem, recv_sem, pair_recv, stale_sem, io_sem, pace_sem, credit_sem,
):
    side = lax.axis_index("side")
    rep = lax.axis_index("rep")
    core = rep % 2
    xpos = (rep // 2) % 2
    ypos = rep // 4
    rank = side % 2
    tokens = hidden.shape[0]
    rows = 2 * LANES

    barrier = pltpu.get_barrier_semaphore()

    def ping(sem, to_side, to_rep):
        pl.semaphore_signal(sem, inc=1, device_id=(to_side, to_rep), device_id_type=MESH)

    x_rep = rep + 2 * (1 - 2 * xpos)
    y_rep = rep + 4 * (1 - 2 * ypos)
    pair_rep = rep + (1 - 2 * core)
    z_side = 5 - side

    def columns(c):
        return pl.ds(pl.multiple_of(c * LANES, LANES), LANES)

    def prompts_in():
        return pltpu.make_async_copy(prompts.at[0, 0], hidden, io_sem.at[0])

    @pl.when(side < 2)
    def _():
        def delta_copies(c):
            slot = weights.at[c, rank, rep // 2, core]

            def copy(src, dst, i):
                return pltpu.make_async_remote_copy(
                    src_ref=src, dst_ref=dst, send_sem=send_sem.at[c % WINDOW, i], recv_sem=own_recv.at[c, i],
                    device_id=(side + 2, rep), device_id_type=MESH,
                )

            return (
                [copy(up_delta.at[pl.ds(i * LANES, LANES), columns(c)], slot.at[i], i) for i in (0, 1)]
                + [copy(down_delta.at[columns(c), pl.ds(i * LANES, LANES)], slot.at[2 + i], 2 + i) for i in (0, 1)]
            )

        prompts_in().start()
        ping(barrier, side + 2, rep)
        ping(barrier, 1 - side, rep)
        pl.semaphore_wait(barrier, 2)

        def sent(c):
            for copy in delta_copies(c):
                copy.wait_send()

        def send(c, carry):
            @pl.when(c >= PACE)
            def _():
                pl.semaphore_wait(credit_sem, 1)

            @pl.when((side == 0) & (c >= 1))
            def _():
                pl.semaphore_wait(pace_sem, 1)

            for copy in delta_copies(c):
                copy.start()

            @pl.when(c >= 1)
            def _():
                sent(c - 1)

            @pl.when((side == 1) & (c >= 1))
            def _():
                ping(pace_sem, 0, rep)

            return carry

        lax.fori_loop(0, n_chunks, send, 0)
        sent(n_chunks - 1)
        prompts_in().wait()
        out = pltpu.make_async_copy(hidden, y_ref.at[0, 0], io_sem.at[1])
        out.start()
        out.wait()

    @pl.when(side >= 2)
    def _():
        prompts_in().start()

        def place(d):
            t = 1 - rank if d & DZ else rank
            yy = 1 - ypos if d & DY else ypos
            xx = 1 - xpos if d & DX else xpos
            return t, yy * 2 + xx

        def stale_copies(c):
            slot = stale.at[c % 2]
            first = pl.multiple_of(rep * rows, rows)

            def part(i):
                return pl.ds(first + i * LANES, LANES)

            return [
                pltpu.make_async_copy(old_up.at[0, 0, 0, part(i), columns(c)], slot.at[i], stale_sem.at[c % 2, i])
                for i in (0, 1)
            ] + [
                pltpu.make_async_copy(
                    old_down.at[0, 0, 0, columns(c), part(i)], slot.at[2 + i], stale_sem.at[c % 2, 2 + i]
                )
                for i in (0, 1)
            ]

        def blocks_of(c, d, blocks):
            t, yx = place(d)
            return weights.at[c, t, yx, core, pl.ds(blocks[0], blocks[1] - blocks[0])]

        def message(c, i):
            d, axis, blocks = SENDS[i]
            ref = blocks_of(c, d, blocks)
            to = {DX: (side, x_rep), DY: (side, y_rep), DZ: (z_side, rep)}[axis]
            return pltpu.make_async_remote_copy(
                src_ref=ref, dst_ref=ref, send_sem=send_sem.at[c % WINDOW, i],
                recv_sem=recv_sem.at[c, ARRIVALS[d | axis, blocks]], device_id=to, device_id_type=MESH,
            )

        def arrived(c, d, blocks):
            ref = blocks_of(c, d, blocks)
            pltpu.make_async_remote_copy(
                src_ref=ref, dst_ref=ref, send_sem=send_sem.at[0, 0], recv_sem=recv_sem.at[c, ARRIVALS[d, blocks]],
                device_id=(side, rep), device_id_type=MESH,
            ).wait_recv()

        def pair_message(c, dz, of_core):
            t = 1 - rank if dz else rank
            ref = weights.at[c, t, :, of_core]
            return pltpu.make_async_remote_copy(
                src_ref=ref, dst_ref=ref, send_sem=send_sem.at[c % WINDOW, len(SENDS) + dz],
                recv_sem=pair_recv.at[c, dz], device_id=(side, pair_rep), device_id_type=MESH,
            )

        for c in (0, 1):
            for copy in stale_copies(c):
                copy.start()
        ping(barrier, side, x_rep)
        ping(barrier, side, y_rep)
        ping(barrier, side, pair_rep)
        ping(barrier, z_side, rep)
        ping(barrier, side - 2, rep)

        def clear(i, carry):
            acc[pl.ds(pl.multiple_of(i * 64, 64), 64), :] = jnp.zeros((64, acc.shape[1]), F32)
            return carry

        lax.fori_loop(0, tokens // 64, clear, 0)
        pl.semaphore_wait(barrier, 5)
        prompts_in().wait()

        def send_all(c, first, last):
            for i in range(first, last):
                message(c, i).start()

        def add_own(c):
            slot = weights.at[c, rank, rep // 2, core]
            for i in range(4):
                pltpu.make_async_remote_copy(
                    src_ref=slot.at[i], dst_ref=slot.at[i], send_sem=send_sem.at[0, 0], recv_sem=own_recv.at[c, i],
                    device_id=(side - 2, rep), device_id_type=MESH,
                ).wait_recv()
            for copy in stale_copies(c):
                copy.wait()
            for i in range(4):
                slot[i] = (stale[c % 2, i].astype(F32) + slot[i].astype(F32)).astype(BF16)

            @pl.when(c + PACE < n_chunks)
            def _():
                ping(credit_sem, side - 2, rep)

            @pl.when(c + 2 < n_chunks)
            def _():
                for copy in stale_copies(c + 2):
                    copy.start()

        half = tokens // 2

        def multiply(c, m):
            here = slice(m * half, (m + 1) * half)
            up_mat = jnp.concatenate(
                [weights[c, t, :, :, 0:2].reshape(acc.shape[1], LANES) for t in (0, 1)], axis=1
            )
            pre_act = jnp.dot(hidden[here, :], up_mat, preferred_element_type=F32)
            act = exact_gelu(pre_act).astype(BF16)
            for piece in range(8):
                down_mat = jnp.concatenate(
                    [
                        jnp.concatenate([weights[c, t, piece // 2, piece % 2, 2 + i] for i in (0, 1)], axis=1)
                        for t in (0, 1)
                    ],
                    axis=0,
                )
                acc[here, piece * rows : (piece + 1) * rows] += jnp.dot(act, down_mat, preferred_element_type=F32)

        def drain(c):
            for i in range(len(SENDS)):
                message(c, i).wait_send()
            for dz in (0, 1):
                pair_message(c, dz, core).wait_send()

        def step(i, carry):
            def during(lag, upto=None):
                if upto is None:
                    return pl.when((i >= lag) & (i < n_chunks + lag))
                return pl.when((i >= lag) & (i < upto + lag))

            @during(0)
            def _():
                add_own(i)
                send_all(i, 0, len(HOP1))

            @during(1)
            def _():
                arrived(i - 1, DZ, WHOLE)
                send_all(i - 1, 3, 5)
                arrived(i - 1, DX, WHOLE)
                arrived(i - 1, DY, WHOLE)
                send_all(i - 1, 5, 7)

            @during(LAST)
            def _():
                for dz in (0, 1):
                    pair_message(i - LAST, dz, 1 - core).wait_recv()
                multiply(i - LAST, 0)

            @during(2)
            def _():
                c = i - 2
                arrived(c, DX | DY, UPPER)
                arrived(c, DX | DY, LOWER)
                send_all(c, 7, len(SENDS))
                pair_message(c, 0, core).start()
                arrived(c, DX | DZ, WHOLE)
                arrived(c, DY | DZ, WHOLE)

            @during(3)
            def _():
                arrived(i - 3, DX | DY | DZ, WHOLE)
                pair_message(i - 3, 1, core).start()

            @during(LAST)
            def _():
                multiply(i - LAST, 1)

            @pl.when((i >= WINDOW - 1) & (i < n_chunks + WINDOW - 1))
            def _():
                drain(i - (WINDOW - 1))

            return carry

        lax.fori_loop(0, n_chunks + LAST, step, 0)
        for c in range(n_chunks + LAST - (WINDOW - 1), n_chunks):
            drain(c)

        finish_rows = tokens // 4

        def result_out(m):
            here = pl.ds(pl.multiple_of(m * finish_rows, finish_rows), finish_rows)
            return pltpu.make_async_copy(hidden.at[here, :], y_ref.at[0, 0, here, :], io_sem.at[m])

        def finish(m, carry):
            here = pl.ds(pl.multiple_of(m * finish_rows, finish_rows), finish_rows)
            hidden[here, :] = (hidden[here, :].astype(F32) + acc[here, :]).astype(BF16)
            result_out(m).start()
            return carry

        lax.fori_loop(0, 4, finish, 0)
        for m in range(4):
            result_out(m).wait()


def solution(mesh):
    up_spec = P("side", None, "rep", None)
    down_spec = P("side", None, None, "rep")
    copy_spec = P("side", "rep", None, None, None)
    token_spec = P("side", "rep", None, None)

    def local_step(w_up, w_down, g_up, g_down, learn_rate, old_up, old_down, prompts):
        step_rate = learn_rate[0]
        new_up = w_up - step_rate * g_up
        new_down = w_down - step_rate * g_down
        delta_up = (new_up - w_up)[0, 0].astype(BF16)
        delta_down = (new_down - w_down)[0, 0].astype(BF16)
        n_chunks = delta_up.shape[1] // LANES
        tokens, model = prompts.shape[2:]
        y = pl.pallas_call(
            functools.partial(sync_kernel, n_chunks),
            out_shape=jax.ShapeDtypeStruct(prompts.shape, BF16),
            in_specs=[pl.BlockSpec(memory_space=pl.ANY)] * 5,
            out_specs=pl.BlockSpec(memory_space=pl.ANY),
            scratch_shapes=[
                pltpu.VMEM((n_chunks, 2, 4, 2, 4, LANES, LANES), BF16),
                pltpu.VMEM((tokens, model), F32),
                pltpu.VMEM((tokens, model), BF16),
                pltpu.VMEM((2, 4, LANES, LANES), BF16),
                pltpu.SemaphoreType.DMA((n_chunks, 4)),
                pltpu.SemaphoreType.DMA((WINDOW, N_SEMS)),
                pltpu.SemaphoreType.DMA((n_chunks, len(ARRIVALS))),
                pltpu.SemaphoreType.DMA((n_chunks, 2)),
                pltpu.SemaphoreType.DMA((2, 4)),
                pltpu.SemaphoreType.DMA((4,)),
                pltpu.SemaphoreType.REGULAR,
                pltpu.SemaphoreType.REGULAR,
            ],
            compiler_params=pltpu.CompilerParams(
                collective_id=0, has_side_effects=True, vmem_limit_bytes=67043328
            ),
        )(delta_up, delta_down, old_up, old_down, prompts)
        return new_up, new_down, y

    return jax.shard_map(
        local_step,
        mesh=mesh,
        in_specs=(up_spec, down_spec, up_spec, down_spec, P(None), copy_spec, copy_spec, token_spec),
        out_specs=(up_spec, down_spec, token_spec),
        check_vma=False,
    )
```

```python
import functools

import jax
import jax.numpy as jnp
from jax import lax
from jax.experimental import pallas as pl
from jax.experimental.pallas import tpu as pltpu
from jax.sharding import PartitionSpec as P

MESH = pl.DeviceIdType.MESH
F32 = jnp.float32
BF16 = jnp.bfloat16
LANES = 128
DX, DY, DZ = 1, 2, 4
WHOLE, UPPER, LOWER = (0, 4), (0, 2), (2, 4)
ARRIVALS = {
    (DX, WHOLE): 0, (DY, WHOLE): 1, (DZ, WHOLE): 2, (DX | DZ, WHOLE): 3, (DY | DZ, WHOLE): 4,
    (DX | DY, UPPER): 5, (DX | DY, LOWER): 6, (DX | DY | DZ, UPPER): 7, (DX | DY | DZ, LOWER): 8,
}
HOP1 = ((0, DX, WHOLE), (0, DY, WHOLE), (0, DZ, WHOLE))
HOP2 = ((DZ, DX, WHOLE), (DZ, DY, WHOLE), (DY, DX, UPPER), (DX, DY, LOWER))
HOP3 = ((DX | DY, DZ, UPPER), (DX | DY, DZ, LOWER))
HOP3_X, HOP3_Y = (DY | DZ, DX, LOWER), (DX | DZ, DY, LOWER)
SENDS = HOP1 + HOP2 + HOP3
N_SEMS = len(SENDS) + 2
WINDOW = 8
PACE = 2
EARLY = 10
LAST = 5


def exact_gelu(v):
    return (0.5 * v) * (1.0 + lax.erf(v * (0.5**0.5)))


def sync_kernel(
    n_chunks, up_delta, down_delta, old_up, old_down, prompts, y_ref,
    weights, acc, hidden, stale,
    own_recv, send_sem, recv_sem, pair_recv, stale_sem, io_sem, pace_sem, credit_sem,
):
    side = lax.axis_index("side")
    rep = lax.axis_index("rep")
    core = rep % 2
    xpos = (rep // 2) % 2
    ypos = rep // 4
    rank = side % 2
    tokens = hidden.shape[0]
    rows = 2 * LANES

    barrier = pltpu.get_barrier_semaphore()

    def ping(sem, to_side, to_rep):
        pl.semaphore_signal(sem, inc=1, device_id=(to_side, to_rep), device_id_type=MESH)

    x_rep = rep + 2 * (1 - 2 * xpos)
    y_rep = rep + 4 * (1 - 2 * ypos)
    pair_rep = rep + (1 - 2 * core)
    z_side = 5 - side

    def columns(c):
        return pl.ds(pl.multiple_of(c * LANES, LANES), LANES)

    def prompts_in():
        return pltpu.make_async_copy(prompts.at[0, 0], hidden, io_sem.at[0])

    @pl.when(side < 2)
    def _():
        def delta_copies(c):
            slot = weights.at[c, rank, rep // 2, core]

            def copy(src, dst, i):
                return pltpu.make_async_remote_copy(
                    src_ref=src, dst_ref=dst, send_sem=send_sem.at[c % WINDOW, i], recv_sem=own_recv.at[c, i],
                    device_id=(side + 2, rep), device_id_type=MESH,
                )

            return (
                [copy(up_delta.at[pl.ds(i * LANES, LANES), columns(c)], slot.at[i], i) for i in (0, 1)]
                + [copy(down_delta.at[columns(c), pl.ds(i * LANES, LANES)], slot.at[2 + i], 2 + i) for i in (0, 1)]
            )

        prompts_in().start()
        ping(barrier, side + 2, rep)
        ping(barrier, 1 - side, rep)
        pl.semaphore_wait(barrier, 2)

        def sent(c):
            for copy in delta_copies(c):
                copy.wait_send()

        def send(c, carry):
            @pl.when(c >= PACE)
            def _():
                pl.semaphore_wait(credit_sem, 1)

            @pl.when((side == 0) & (c >= 1))
            def _():
                pl.semaphore_wait(pace_sem, 1)

            for copy in delta_copies(c):
                copy.start()

            @pl.when(c >= 1)
            def _():
                sent(c - 1)

            @pl.when((side == 1) & (c >= 1))
            def _():
                ping(pace_sem, 0, rep)

            return carry

        lax.fori_loop(0, n_chunks, send, 0)
        sent(n_chunks - 1)
        prompts_in().wait()
        out = pltpu.make_async_copy(hidden, y_ref.at[0, 0], io_sem.at[1])
        out.start()
        out.wait()

    @pl.when(side >= 2)
    def _():
        prompts_in().start()

        def place(d):
            t = 1 - rank if d & DZ else rank
            yy = 1 - ypos if d & DY else ypos
            xx = 1 - xpos if d & DX else xpos
            return t, yy * 2 + xx

        def stale_copies(c):
            slot = stale.at[c % 2]
            first = pl.multiple_of(rep * rows, rows)

            def part(i):
                return pl.ds(first + i * LANES, LANES)

            return [
                pltpu.make_async_copy(old_up.at[0, 0, 0, part(i), columns(c)], slot.at[i], stale_sem.at[c % 2, i])
                for i in (0, 1)
            ] + [
                pltpu.make_async_copy(
                    old_down.at[0, 0, 0, columns(c), part(i)], slot.at[2 + i], stale_sem.at[c % 2, 2 + i]
                )
                for i in (0, 1)
            ]

        def blocks_of(c, d, blocks):
            t, yx = place(d)
            return weights.at[c, t, yx, core, pl.ds(blocks[0], blocks[1] - blocks[0])]

        def message(c, i, route=None):
            d, axis, blocks = route or SENDS[i]
            ref = blocks_of(c, d, blocks)
            to = {DX: (side, x_rep), DY: (side, y_rep), DZ: (z_side, rep)}[axis]
            return pltpu.make_async_remote_copy(
                src_ref=ref, dst_ref=ref, send_sem=send_sem.at[c % WINDOW, i],
                recv_sem=recv_sem.at[c, ARRIVALS[d | axis, blocks]], device_id=to, device_id_type=MESH,
            )

        def arrived(c, d, blocks):
            ref = blocks_of(c, d, blocks)
            pltpu.make_async_remote_copy(
                src_ref=ref, dst_ref=ref, send_sem=send_sem.at[0, 0], recv_sem=recv_sem.at[c, ARRIVALS[d, blocks]],
                device_id=(side, rep), device_id_type=MESH,
            ).wait_recv()

        def pair_message(c, dz, of_core):
            t = 1 - rank if dz else rank
            ref = weights.at[c, t, :, of_core]
            return pltpu.make_async_remote_copy(
                src_ref=ref, dst_ref=ref, send_sem=send_sem.at[c % WINDOW, len(SENDS) + dz],
                recv_sem=pair_recv.at[c, dz], device_id=(side, pair_rep), device_id_type=MESH,
            )

        for c in (0, 1):
            for copy in stale_copies(c):
                copy.start()
        ping(barrier, side, x_rep)
        ping(barrier, side, y_rep)
        ping(barrier, side, pair_rep)
        ping(barrier, z_side, rep)
        ping(barrier, side - 2, rep)

        prompts_in().wait()

        def residual(i, carry):
            here = pl.ds(pl.multiple_of(i * 64, 64), 64)
            acc[here, :] = hidden[here, :].astype(F32)
            return carry

        lax.fori_loop(0, tokens // 64, residual, 0)
        pl.semaphore_wait(barrier, 5)

        def send_all(c, first, last):
            for i in range(first, last):
                message(c, i).start()

        def add_own(c):
            slot = weights.at[c, rank, rep // 2, core]
            for i in range(4):
                pltpu.make_async_remote_copy(
                    src_ref=slot.at[i], dst_ref=slot.at[i], send_sem=send_sem.at[0, 0], recv_sem=own_recv.at[c, i],
                    device_id=(side - 2, rep), device_id_type=MESH,
                ).wait_recv()
            for copy in stale_copies(c):
                copy.wait()
            for i in range(4):
                slot[i] = (stale[c % 2, i].astype(F32) + slot[i].astype(F32)).astype(BF16)

            @pl.when(c + PACE < n_chunks)
            def _():
                ping(credit_sem, side - 2, rep)

            @pl.when(c + 2 < n_chunks)
            def _():
                for copy in stale_copies(c + 2):
                    copy.start()

        half = tokens // 2

        def multiply(c, m):
            here = slice(m * half, (m + 1) * half)
            up_mat = jnp.concatenate(
                [weights[c, t, :, :, 0:2].reshape(acc.shape[1], LANES) for t in (0, 1)], axis=1
            )
            pre_act = jnp.dot(hidden[here, :], up_mat, preferred_element_type=F32)
            act = exact_gelu(pre_act).astype(BF16)
            for piece in range(8):
                down_mat = jnp.concatenate(
                    [
                        jnp.concatenate([weights[c, t, piece // 2, piece % 2, 2 + i] for i in (0, 1)], axis=1)
                        for t in (0, 1)
                    ],
                    axis=0,
                )
                acc[here, piece * rows : (piece + 1) * rows] += jnp.dot(act, down_mat, preferred_element_type=F32)

        def drain(c):
            for i in range(len(SENDS)):
                message(c, i).wait_send()
            for dz in (0, 1):
                pair_message(c, dz, core).wait_send()

        def step(i, carry):
            def during(lag):
                return pl.when((i >= lag) & (i < n_chunks + lag))

            @during(0)
            def _():
                add_own(i)
                send_all(i, 0, 3)

            @during(3)
            def _():
                c = i - 3
                arrived(c, DX | DY, UPPER)
                arrived(c, DX | DY, LOWER)
                arrived(c, DX | DZ, WHOLE)
                arrived(c, DY | DZ, WHOLE)
                message(c, 7).start()
                early = c < EARLY

                @pl.when(early & (c % 2 == 1))
                def _():
                    message(c, 8, HOP3_X).start()

                @pl.when(early & (c % 2 == 0))
                def _():
                    message(c, 8, HOP3_Y).start()

                @pl.when(c >= EARLY)
                def _():
                    message(c, 8).start()

            @during(1)
            def _():
                arrived(i - 1, DZ, WHOLE)
                send_all(i - 1, 3, 5)

            @during(3)
            def _():
                pair_message(i - 3, 0, core).start()

            @during(LAST)
            def _():
                for dz in (0, 1):
                    pair_message(i - LAST, dz, 1 - core).wait_recv()
                multiply(i - LAST, 0)

            @during(1)
            def _():
                arrived(i - 1, DX, WHOLE)
                arrived(i - 1, DY, WHOLE)
                send_all(i - 1, 5, 7)

            @during(4)
            def _():
                arrived(i - 4, DX | DY | DZ, UPPER)
                arrived(i - 4, DX | DY | DZ, LOWER)
                pair_message(i - 4, 1, core).start()

            @during(LAST)
            def _():
                multiply(i - LAST, 1)

            @pl.when((i >= WINDOW - 1) & (i < n_chunks + WINDOW - 1))
            def _():
                drain(i - (WINDOW - 1))

            return carry

        lax.fori_loop(0, n_chunks + LAST, step, 0)
        for c in range(n_chunks + LAST - (WINDOW - 1), n_chunks):
            drain(c)

        finish_rows = tokens // 4

        def result_out(m):
            here = pl.ds(pl.multiple_of(m * finish_rows, finish_rows), finish_rows)
            return pltpu.make_async_copy(hidden.at[here, :], y_ref.at[0, 0, here, :], io_sem.at[m])

        def finish(m, carry):
            here = pl.ds(pl.multiple_of(m * finish_rows, finish_rows), finish_rows)
            hidden[here, :] = acc[here, :].astype(BF16)
            result_out(m).start()
            return carry

        lax.fori_loop(0, 4, finish, 0)
        for m in range(4):
            result_out(m).wait()


def solution(mesh):
    up_spec = P("side", None, "rep", None)
    down_spec = P("side", None, None, "rep")
    copy_spec = P("side", "rep", None, None, None)
    token_spec = P("side", "rep", None, None)

    def local_step(w_up, w_down, g_up, g_down, learn_rate, old_up, old_down, prompts):
        step_rate = learn_rate[0]
        new_up = w_up - step_rate * g_up
        new_down = w_down - step_rate * g_down
        delta_up = (new_up - w_up)[0, 0].astype(BF16)
        delta_down = (new_down - w_down)[0, 0].astype(BF16)
        n_chunks = delta_up.shape[1] // LANES
        tokens, model = prompts.shape[2:]
        y = pl.pallas_call(
            functools.partial(sync_kernel, n_chunks),
            out_shape=jax.ShapeDtypeStruct(prompts.shape, BF16),
            in_specs=[pl.BlockSpec(memory_space=pl.ANY)] * 5,
            out_specs=pl.BlockSpec(memory_space=pl.ANY),
            scratch_shapes=[
                pltpu.VMEM((n_chunks, 2, 4, 2, 4, LANES, LANES), BF16),
                pltpu.VMEM((tokens, model), F32),
                pltpu.VMEM((tokens, model), BF16),
                pltpu.VMEM((2, 4, LANES, LANES), BF16),
                pltpu.SemaphoreType.DMA((n_chunks, 4)),
                pltpu.SemaphoreType.DMA((WINDOW, N_SEMS)),
                pltpu.SemaphoreType.DMA((n_chunks, len(ARRIVALS))),
                pltpu.SemaphoreType.DMA((n_chunks, 2)),
                pltpu.SemaphoreType.DMA((2, 4)),
                pltpu.SemaphoreType.DMA((4,)),
                pltpu.SemaphoreType.REGULAR,
                pltpu.SemaphoreType.REGULAR,
            ],
            compiler_params=pltpu.CompilerParams(
                collective_id=0, has_side_effects=True, vmem_limit_bytes=67043328
            ),
        )(delta_up, delta_down, old_up, old_down, prompts)
        return new_up, new_down, y

    return jax.shard_map(
        local_step,
        mesh=mesh,
        in_specs=(up_spec, down_spec, up_spec, down_spec, P(None), copy_spec, copy_spec, token_spec),
        out_specs=(up_spec, down_spec, token_spec),
        check_vma=False,
    )
```

```python
import functools

import jax
import jax.numpy as jnp
from jax import lax
from jax.experimental import pallas as pl
from jax.experimental.pallas import tpu as pltpu
from jax.sharding import PartitionSpec as P

MESH = pl.DeviceIdType.MESH
F32 = jnp.float32
BF16 = jnp.bfloat16
LANES = 128
DX, DY, DZ = 1, 2, 4
WHOLE, UPPER, LOWER = (0, 4), (0, 2), (2, 4)
ARRIVALS = {
    (DX, WHOLE): 0, (DY, WHOLE): 1, (DZ, WHOLE): 2, (DX | DZ, WHOLE): 3, (DY | DZ, WHOLE): 4,
    (DX | DY, UPPER): 5, (DX | DY, LOWER): 6, (DX | DY | DZ, UPPER): 7, (DX | DY | DZ, LOWER): 8,
}
HOP1 = ((0, DX, WHOLE), (0, DY, WHOLE), (0, DZ, WHOLE))
HOP2 = ((DZ, DX, WHOLE), (DZ, DY, WHOLE), (DY, DX, UPPER), (DX, DY, LOWER))
HOP3 = ((DX | DY, DZ, UPPER), (DX | DY, DZ, LOWER))
HOP3_X, HOP3_Y = (DY | DZ, DX, LOWER), (DX | DZ, DY, LOWER)
SENDS = HOP1 + HOP2 + HOP3
N_SEMS = len(SENDS) + 2
WINDOW = 8
PACE = 2
EARLY = 10
LAST = 5
VMEM_BYTES = 58 * 2**20


def exact_gelu(v):
    return (0.5 * v) * (1.0 + lax.erf(v * (0.5**0.5)))


def sync_kernel(
    n_chunks, learn_rate, w_up, w_down, g_up, g_down, old_up, old_down, prompts, zeroed_up, zeroed_down, hidden,
    weights, acc, stale, up_pair, down_pair,
    own_recv, send_sem, recv_sem, pair_recv, stale_sem, fetch_sem, io_sem, pace_sem, credit_sem,
):
    side = lax.axis_index("side")
    rep = lax.axis_index("rep")
    core = rep % 2
    xpos = (rep // 2) % 2
    ypos = rep // 4
    rank = side % 2
    tokens = hidden.shape[0]
    rows = 2 * LANES
    del zeroed_up, zeroed_down

    barrier = pltpu.get_barrier_semaphore()

    def ping(sem, to_side, to_rep):
        pl.semaphore_signal(sem, inc=1, device_id=(to_side, to_rep), device_id_type=MESH)

    x_rep = rep + 2 * (1 - 2 * xpos)
    y_rep = rep + 4 * (1 - 2 * ypos)
    pair_rep = rep + (1 - 2 * core)
    z_side = 5 - side

    def columns(c):
        return pl.ds(pl.multiple_of(c * LANES, LANES), LANES)

    def prompts_in():
        return pltpu.make_async_copy(prompts.at[0, 0], hidden, io_sem)

    @pl.when(side < 2)
    def _():
        def fetches(c):
            slot = c % 2
            return [
                pltpu.make_async_copy(src, dst, fetch_sem.at[slot, i])
                for i, (src, dst) in enumerate(
                    (
                        (w_up.at[0, 0, :, columns(c)], up_pair.at[slot, 0]),
                        (g_up.at[0, 0, :, columns(c)], up_pair.at[slot, 1]),
                        (w_down.at[0, 0, columns(c), :], down_pair.at[slot, 0]),
                        (g_down.at[0, 0, columns(c), :], down_pair.at[slot, 1]),
                    )
                )
            ]

        def fetch(c):
            for copy in fetches(c):
                copy.start()

        def prepare(c):
            for copy in fetches(c):
                copy.wait()
            rate = learn_rate[0]
            slot = weights.at[c, rank, rep // 2, core]
            for i in (0, 1):
                part = slice(i * LANES, (i + 1) * LANES)
                for j, pair, here in ((0, up_pair, (part, slice(None))), (2, down_pair, (slice(None), part))):
                    old = pair[(c % 2, 0) + here]
                    slot[j + i] = ((old - rate * pair[(c % 2, 1) + here]) - old).astype(BF16)

        def delta_copy(c):
            ref = weights.at[c, rank, rep // 2, core]
            return pltpu.make_async_remote_copy(
                src_ref=ref, dst_ref=ref, send_sem=send_sem.at[c % WINDOW, 0], recv_sem=own_recv.at[c],
                device_id=(side + 2, rep), device_id_type=MESH,
            )

        fetch(0)
        fetch(1)
        prompts_in().start()
        ping(barrier, side + 2, rep)
        ping(barrier, 1 - side, rep)
        for c in (0, 1):
            prepare(c)
            fetch(c + 2)
        pl.semaphore_wait(barrier, 2)

        def send(c, carry):
            @pl.when(c >= PACE)
            def _():
                pl.semaphore_wait(credit_sem, 1)

            @pl.when((side == 0) & (c >= 1))
            def _():
                pl.semaphore_wait(pace_sem, 1)

            delta_copy(c).start()

            @pl.when(c + 2 < n_chunks)
            def _():
                prepare(c + 2)

            @pl.when(c + 4 < n_chunks)
            def _():
                fetch(c + 4)

            @pl.when(c >= 1)
            def _():
                delta_copy(c - 1).wait_send()

            @pl.when((side == 1) & (c >= 1))
            def _():
                ping(pace_sem, 0, rep)

            return carry

        lax.fori_loop(0, n_chunks, send, 0)
        delta_copy(n_chunks - 1).wait_send()
        prompts_in().wait()

    @pl.when(side >= 2)
    def _():
        prompts_in().start()

        def place(d):
            t = 1 - rank if d & DZ else rank
            yy = 1 - ypos if d & DY else ypos
            xx = 1 - xpos if d & DX else xpos
            return t, yy * 2 + xx

        def stale_copies(c):
            slot = stale.at[c % 2]
            first = pl.multiple_of(rep * rows, rows)

            def part(i):
                return pl.ds(first + i * LANES, LANES)

            return [
                pltpu.make_async_copy(old_up.at[0, 0, 0, part(i), columns(c)], slot.at[i], stale_sem.at[c % 2, i])
                for i in (0, 1)
            ] + [
                pltpu.make_async_copy(
                    old_down.at[0, 0, 0, columns(c), part(i)], slot.at[2 + i], stale_sem.at[c % 2, 2 + i]
                )
                for i in (0, 1)
            ]

        def blocks_of(c, d, blocks):
            t, yx = place(d)
            return weights.at[c, t, yx, core, pl.ds(blocks[0], blocks[1] - blocks[0])]

        def message(c, i, route=None):
            d, axis, blocks = route or SENDS[i]
            ref = blocks_of(c, d, blocks)
            to = {DX: (side, x_rep), DY: (side, y_rep), DZ: (z_side, rep)}[axis]
            return pltpu.make_async_remote_copy(
                src_ref=ref, dst_ref=ref, send_sem=send_sem.at[c % WINDOW, i],
                recv_sem=recv_sem.at[c, ARRIVALS[d | axis, blocks]], device_id=to, device_id_type=MESH,
            )

        def arrived(c, d, blocks):
            ref = blocks_of(c, d, blocks)
            pltpu.make_async_remote_copy(
                src_ref=ref, dst_ref=ref, send_sem=send_sem.at[0, 0], recv_sem=recv_sem.at[c, ARRIVALS[d, blocks]],
                device_id=(side, rep), device_id_type=MESH,
            ).wait_recv()

        def pair_message(c, dz, of_core):
            t = 1 - rank if dz else rank
            ref = weights.at[c, t, :, of_core]
            return pltpu.make_async_remote_copy(
                src_ref=ref, dst_ref=ref, send_sem=send_sem.at[c % WINDOW, len(SENDS) + dz],
                recv_sem=pair_recv.at[c, dz], device_id=(side, pair_rep), device_id_type=MESH,
            )

        for c in (0, 1):
            for copy in stale_copies(c):
                copy.start()
        ping(barrier, side, x_rep)
        ping(barrier, side, y_rep)
        ping(barrier, side, pair_rep)
        ping(barrier, z_side, rep)
        ping(barrier, side - 2, rep)

        prompts_in().wait()

        def residual(i, carry):
            here = pl.ds(pl.multiple_of(i * 64, 64), 64)
            acc[here, :] = hidden[here, :].astype(F32)
            return carry

        lax.fori_loop(0, tokens // 64, residual, 0)
        pl.semaphore_wait(barrier, 5)

        def send_all(c, first, last):
            for i in range(first, last):
                message(c, i).start()

        def add_own(c):
            slot = weights.at[c, rank, rep // 2, core]
            pltpu.make_async_remote_copy(
                src_ref=slot, dst_ref=slot, send_sem=send_sem.at[0, 0], recv_sem=own_recv.at[c],
                device_id=(side - 2, rep), device_id_type=MESH,
            ).wait_recv()
            for copy in stale_copies(c):
                copy.wait()
            for i in range(4):
                slot[i] = (stale[c % 2, i].astype(F32) + slot[i].astype(F32)).astype(BF16)

            @pl.when(c + PACE < n_chunks)
            def _():
                ping(credit_sem, side - 2, rep)

            @pl.when(c + 2 < n_chunks)
            def _():
                for copy in stale_copies(c + 2):
                    copy.start()

        half = tokens // 2

        def multiply(c, m):
            here = slice(m * half, (m + 1) * half)
            up_mat = jnp.concatenate(
                [weights[c, t, :, :, 0:2].reshape(acc.shape[1], LANES) for t in (0, 1)], axis=1
            )
            pre_act = jnp.dot(hidden[here, :], up_mat, preferred_element_type=F32)
            act = exact_gelu(pre_act).astype(BF16)
            for piece in range(8):
                down_mat = jnp.concatenate(
                    [
                        jnp.concatenate([weights[c, t, piece // 2, piece % 2, 2 + i] for i in (0, 1)], axis=1)
                        for t in (0, 1)
                    ],
                    axis=0,
                )
                acc[here, piece * rows : (piece + 1) * rows] += jnp.dot(act, down_mat, preferred_element_type=F32)

        def drain(c):
            for i in range(len(SENDS)):
                message(c, i).wait_send()
            for dz in (0, 1):
                pair_message(c, dz, core).wait_send()

        def step(i, carry):
            def during(lag):
                return pl.when((i >= lag) & (i < n_chunks + lag))

            @during(0)
            def _():
                add_own(i)
                send_all(i, 0, 3)

            @during(3)
            def _():
                c = i - 3
                arrived(c, DX | DY, UPPER)
                arrived(c, DX | DY, LOWER)
                arrived(c, DX | DZ, WHOLE)
                arrived(c, DY | DZ, WHOLE)
                message(c, 7).start()
                early = c < EARLY

                @pl.when(early & (c % 2 == 1))
                def _():
                    message(c, 8, HOP3_X).start()

                @pl.when(early & (c % 2 == 0))
                def _():
                    message(c, 8, HOP3_Y).start()

                @pl.when(c >= EARLY)
                def _():
                    message(c, 8).start()

            @during(1)
            def _():
                arrived(i - 1, DZ, WHOLE)
                send_all(i - 1, 3, 5)

            @during(3)
            def _():
                pair_message(i - 3, 0, core).start()

            @during(LAST)
            def _():
                for dz in (0, 1):
                    pair_message(i - LAST, dz, 1 - core).wait_recv()
                multiply(i - LAST, 0)

            @during(1)
            def _():
                arrived(i - 1, DX, WHOLE)
                arrived(i - 1, DY, WHOLE)
                send_all(i - 1, 5, 7)

            @during(4)
            def _():
                arrived(i - 4, DX | DY | DZ, UPPER)
                arrived(i - 4, DX | DY | DZ, LOWER)
                pair_message(i - 4, 1, core).start()

            @during(LAST)
            def _():
                multiply(i - LAST, 1)

            @pl.when((i >= WINDOW - 1) & (i < n_chunks + WINDOW - 1))
            def _():
                drain(i - (WINDOW - 1))

            return carry

        lax.fori_loop(0, n_chunks + LAST, step, 0)
        for c in range(n_chunks + LAST - (WINDOW - 1), n_chunks):
            drain(c)

        def finish(i, carry):
            here = pl.ds(pl.multiple_of(i * 64, 64), 64)
            hidden[here, :] = acc[here, :].astype(BF16)
            return carry

        lax.fori_loop(0, tokens // 64, finish, 0)


def zero_kernel(up_ref, down_ref, zeros, sems):
    @pl.when(lax.axis_index("side") >= 2)
    def _():
        zeros[...] = jnp.zeros_like(zeros)
        copies = []
        for n, ref in enumerate((up_ref.at[0, 0], down_ref.at[0, 0])):
            high, wide = ref.shape
            for i in range(high // zeros.shape[0]):
                for j in range(wide // zeros.shape[1]):
                    part = ref.at[pl.ds(i * zeros.shape[0], zeros.shape[0]), pl.ds(j * zeros.shape[1], zeros.shape[1])]
                    copies.append(pltpu.make_async_copy(zeros, part, sems.at[n]))
        for copy in copies:
            copy.start()
        for copy in copies:
            copy.wait()


def last_kernel(learn_rate, w_up, w_down, g_up, g_down, up_in, down_in, hidden, up_out, down_out, y_ref, sem):
    del up_in, down_in
    result = pltpu.make_async_copy(hidden, y_ref.at[0, 0], sem)
    result.start()

    @pl.when(lax.axis_index("side") < 2)
    def _():
        rate = learn_rate[0]

        def body(w, g, out):
            out[...] = w[...] - rate * g[...]

        for w, g, out in ((w_up, g_up, up_out), (w_down, g_down, down_out)):
            high, wide = w.shape[2:]
            spec = pl.BlockSpec((high // 8, wide), lambda i: (i, 0))
            pltpu.emit_pipeline(body, grid=(8,), in_specs=[spec, spec], out_specs=[spec])(
                w.at[0, 0], g.at[0, 0], out.at[0, 0]
            )

    result.wait()


def solution(mesh):
    up_spec = P("side", None, "rep", None)
    down_spec = P("side", None, None, "rep")
    copy_spec = P("side", "rep", None, None, None)
    token_spec = P("side", "rep", None, None)

    def local_step(w_up, w_down, g_up, g_down, learn_rate, old_up, old_down, prompts):
        n_chunks = w_up.shape[3] // LANES
        tokens, model = prompts.shape[2:]
        rows = w_up.shape[2]
        anywhere = pl.BlockSpec(memory_space=pl.ANY)
        scalar = pl.BlockSpec(memory_space=pltpu.SMEM)
        on_chip = pl.BlockSpec(memory_space=pltpu.VMEM)
        new_shapes = [jax.ShapeDtypeStruct(w.shape, F32) for w in (w_up, w_down)]
        zero_up, zero_down = pl.pallas_call(
            zero_kernel,
            out_shape=new_shapes,
            out_specs=[anywhere] * 2,
            scratch_shapes=[pltpu.VMEM((256, 256), F32), pltpu.SemaphoreType.DMA((2,))],
            compiler_params=pltpu.CompilerParams(has_side_effects=True, vmem_limit_bytes=32 * 2**20),
        )()
        hidden = pl.pallas_call(
            functools.partial(sync_kernel, n_chunks),
            out_shape=pltpu.VMEM((tokens, model), BF16),
            in_specs=[scalar] + [anywhere] * 9,
            out_specs=on_chip,
            scratch_shapes=[
                pltpu.VMEM((n_chunks, 2, 4, 2, 4, LANES, LANES), BF16),
                pltpu.VMEM((tokens, model), F32),
                pltpu.VMEM((2, 4, LANES, LANES), BF16),
                pltpu.VMEM((2, 2, rows, LANES), F32),
                pltpu.VMEM((2, 2, LANES, rows), F32),
                pltpu.SemaphoreType.DMA((n_chunks,)),
                pltpu.SemaphoreType.DMA((WINDOW, N_SEMS)),
                pltpu.SemaphoreType.DMA((n_chunks, len(ARRIVALS))),
                pltpu.SemaphoreType.DMA((n_chunks, 2)),
                pltpu.SemaphoreType.DMA((2, 4)),
                pltpu.SemaphoreType.DMA((2, 4)),
                pltpu.SemaphoreType.DMA,
                pltpu.SemaphoreType.REGULAR,
                pltpu.SemaphoreType.REGULAR,
            ],
            compiler_params=pltpu.CompilerParams(
                collective_id=0, has_side_effects=True, vmem_limit_bytes=VMEM_BYTES
            ),
        )(learn_rate, w_up, w_down, g_up, g_down, old_up, old_down, prompts, zero_up, zero_down)
        return pl.pallas_call(
            last_kernel,
            out_shape=new_shapes + [jax.ShapeDtypeStruct(prompts.shape, BF16)],
            in_specs=[scalar] + [anywhere] * 6 + [on_chip],
            out_specs=[anywhere] * 3,
            input_output_aliases={5: 0, 6: 1},
            scratch_shapes=[pltpu.SemaphoreType.DMA],
            compiler_params=pltpu.CompilerParams(vmem_limit_bytes=VMEM_BYTES),
        )(
            learn_rate, w_up, w_down, g_up, g_down, zero_up, zero_down,
            pltpu.with_memory_space_constraint(hidden, pltpu.VMEM),
        )

    return jax.shard_map(
        local_step,
        mesh=mesh,
        in_specs=(up_spec, down_spec, up_spec, down_spec, P(None), copy_spec, copy_spec, token_spec),
        out_specs=(up_spec, down_spec, token_spec),
        check_vma=False,
    )
```

```python
import functools

import jax
import jax.numpy as jnp
from jax import lax
from jax.experimental import pallas as pl
from jax.experimental.pallas import tpu as pltpu
from jax.sharding import PartitionSpec as P

MESH = pl.DeviceIdType.MESH
F32 = jnp.float32
BF16 = jnp.bfloat16
LANES = 128
DX, DY, DZ = 1, 2, 4
WHOLE, UPPER, LOWER = (0, 4), (0, 2), (2, 4)
ARRIVALS = {
    (DX, WHOLE): 0, (DY, WHOLE): 1, (DZ, WHOLE): 2, (DX | DZ, WHOLE): 3, (DY | DZ, WHOLE): 4,
    (DX | DY, UPPER): 5, (DX | DY, LOWER): 6, (DX | DY | DZ, UPPER): 7, (DX | DY | DZ, LOWER): 8,
}
HOP1 = ((0, DX, WHOLE), (0, DY, WHOLE), (0, DZ, WHOLE))
HOP2 = ((DZ, DX, WHOLE), (DZ, DY, WHOLE), (DY, DX, UPPER), (DX, DY, LOWER))
HOP3 = ((DX | DY, DZ, UPPER), (DX | DY, DZ, LOWER))
HOP3_X, HOP3_Y = (DY | DZ, DX, LOWER), (DX | DZ, DY, LOWER)
SENDS = HOP1 + HOP2 + HOP3
N_SEMS = len(SENDS) + 2
WINDOW = 8
PACE = 2
EARLY = 10
LAST = 5
VMEM_BYTES = 54 * 2**20
FINISH = 64


def exact_gelu(v):
    return (0.5 * v) * (1.0 + lax.erf(v * (0.5**0.5)))


def sync_kernel(
    n_chunks, learn_rate, w_up, w_down, g_up, g_down, old_up, old_down, prompts, acc,
    weights, hidden, stale, up_pair, down_pair,
    own_recv, send_sem, recv_sem, pair_recv, stale_sem, fetch_sem, io_sem, pace_sem, credit_sem,
):
    side = lax.axis_index("side")
    rep = lax.axis_index("rep")
    core = rep % 2
    xpos = (rep // 2) % 2
    ypos = rep // 4
    rank = side % 2
    tokens = hidden.shape[0]
    rows = 2 * LANES

    barrier = pltpu.get_barrier_semaphore()

    def ping(sem, to_side, to_rep):
        pl.semaphore_signal(sem, inc=1, device_id=(to_side, to_rep), device_id_type=MESH)

    x_rep = rep + 2 * (1 - 2 * xpos)
    y_rep = rep + 4 * (1 - 2 * ypos)
    pair_rep = rep + (1 - 2 * core)
    z_side = 5 - side

    def columns(c):
        return pl.ds(pl.multiple_of(c * LANES, LANES), LANES)

    def prompts_in():
        return pltpu.make_async_copy(prompts.at[0, 0], hidden, io_sem)

    def residual(i, carry):
        here = pl.ds(pl.multiple_of(i * 64, 64), 64)
        acc[here, :] = hidden[here, :].astype(F32)
        return carry

    @pl.when(side < 2)
    def _():
        def fetches(c):
            slot = c % 2
            return [
                pltpu.make_async_copy(src, dst, fetch_sem.at[slot, i])
                for i, (src, dst) in enumerate(
                    (
                        (w_up.at[0, 0, :, columns(c)], up_pair.at[slot, 0]),
                        (g_up.at[0, 0, :, columns(c)], up_pair.at[slot, 1]),
                        (w_down.at[0, 0, columns(c), :], down_pair.at[slot, 0]),
                        (g_down.at[0, 0, columns(c), :], down_pair.at[slot, 1]),
                    )
                )
            ]

        def fetch(c):
            for copy in fetches(c):
                copy.start()

        def prepare(c):
            for copy in fetches(c):
                copy.wait()
            rate = learn_rate[0]
            slot = weights.at[c, rank, rep // 2, core]
            for i in (0, 1):
                part = slice(i * LANES, (i + 1) * LANES)
                for j, pair, here in ((0, up_pair, (part, slice(None))), (2, down_pair, (slice(None), part))):
                    old = pair[(c % 2, 0) + here]
                    slot[j + i] = ((old - rate * pair[(c % 2, 1) + here]) - old).astype(BF16)

        def delta_copy(c):
            ref = weights.at[c, rank, rep // 2, core]
            return pltpu.make_async_remote_copy(
                src_ref=ref, dst_ref=ref, send_sem=send_sem.at[c % WINDOW, 0], recv_sem=own_recv.at[c],
                device_id=(side + 2, rep), device_id_type=MESH,
            )

        fetch(0)
        fetch(1)
        prompts_in().start()
        ping(barrier, side + 2, rep)
        ping(barrier, 1 - side, rep)
        for c in (0, 1):
            prepare(c)
            fetch(c + 2)
        pl.semaphore_wait(barrier, 2)

        def send(c, carry):
            @pl.when(c >= PACE)
            def _():
                pl.semaphore_wait(credit_sem, 1)

            @pl.when((side == 0) & (c >= 1))
            def _():
                pl.semaphore_wait(pace_sem, 1)

            delta_copy(c).start()

            @pl.when(c + 2 < n_chunks)
            def _():
                prepare(c + 2)

            @pl.when(c + 4 < n_chunks)
            def _():
                fetch(c + 4)

            @pl.when(c >= 1)
            def _():
                delta_copy(c - 1).wait_send()

            @pl.when((side == 1) & (c >= 1))
            def _():
                ping(pace_sem, 0, rep)

            return carry

        lax.fori_loop(0, n_chunks, send, 0)
        delta_copy(n_chunks - 1).wait_send()
        prompts_in().wait()
        lax.fori_loop(0, tokens // 64, residual, 0)

    @pl.when(side >= 2)
    def _():
        prompts_in().start()

        def place(d):
            t = 1 - rank if d & DZ else rank
            yy = 1 - ypos if d & DY else ypos
            xx = 1 - xpos if d & DX else xpos
            return t, yy * 2 + xx

        def stale_copies(c):
            slot = stale.at[c % 2]
            first = pl.multiple_of(rep * rows, rows)

            def part(i):
                return pl.ds(first + i * LANES, LANES)

            return [
                pltpu.make_async_copy(old_up.at[0, 0, 0, part(i), columns(c)], slot.at[i], stale_sem.at[c % 2, i])
                for i in (0, 1)
            ] + [
                pltpu.make_async_copy(
                    old_down.at[0, 0, 0, columns(c), part(i)], slot.at[2 + i], stale_sem.at[c % 2, 2 + i]
                )
                for i in (0, 1)
            ]

        def blocks_of(c, d, blocks):
            t, yx = place(d)
            return weights.at[c, t, yx, core, pl.ds(blocks[0], blocks[1] - blocks[0])]

        def message(c, i, route=None):
            d, axis, blocks = route or SENDS[i]
            ref = blocks_of(c, d, blocks)
            to = {DX: (side, x_rep), DY: (side, y_rep), DZ: (z_side, rep)}[axis]
            return pltpu.make_async_remote_copy(
                src_ref=ref, dst_ref=ref, send_sem=send_sem.at[c % WINDOW, i],
                recv_sem=recv_sem.at[c, ARRIVALS[d | axis, blocks]], device_id=to, device_id_type=MESH,
            )

        def arrived(c, d, blocks):
            ref = blocks_of(c, d, blocks)
            pltpu.make_async_remote_copy(
                src_ref=ref, dst_ref=ref, send_sem=send_sem.at[0, 0], recv_sem=recv_sem.at[c, ARRIVALS[d, blocks]],
                device_id=(side, rep), device_id_type=MESH,
            ).wait_recv()

        def pair_message(c, dz, of_core):
            t = 1 - rank if dz else rank
            ref = weights.at[c, t, :, of_core]
            return pltpu.make_async_remote_copy(
                src_ref=ref, dst_ref=ref, send_sem=send_sem.at[c % WINDOW, len(SENDS) + dz],
                recv_sem=pair_recv.at[c, dz], device_id=(side, pair_rep), device_id_type=MESH,
            )

        for c in (0, 1):
            for copy in stale_copies(c):
                copy.start()
        ping(barrier, side, x_rep)
        ping(barrier, side, y_rep)
        ping(barrier, side, pair_rep)
        ping(barrier, z_side, rep)
        ping(barrier, side - 2, rep)

        prompts_in().wait()
        lax.fori_loop(0, tokens // 64, residual, 0)
        pl.semaphore_wait(barrier, 5)

        def send_all(c, first, last):
            for i in range(first, last):
                message(c, i).start()

        def add_own(c):
            slot = weights.at[c, rank, rep // 2, core]
            pltpu.make_async_remote_copy(
                src_ref=slot, dst_ref=slot, send_sem=send_sem.at[0, 0], recv_sem=own_recv.at[c],
                device_id=(side - 2, rep), device_id_type=MESH,
            ).wait_recv()
            for copy in stale_copies(c):
                copy.wait()
            for i in range(4):
                slot[i] = (stale[c % 2, i].astype(F32) + slot[i].astype(F32)).astype(BF16)

            @pl.when(c + PACE < n_chunks)
            def _():
                ping(credit_sem, side - 2, rep)

            @pl.when(c + 2 < n_chunks)
            def _():
                for copy in stale_copies(c + 2):
                    copy.start()

        half = tokens // 2

        def multiply(c, m):
            here = slice(m * half, (m + 1) * half)
            up_mat = jnp.concatenate(
                [weights[c, t, :, :, 0:2].reshape(acc.shape[1], LANES) for t in (0, 1)], axis=1
            )
            pre_act = jnp.dot(hidden[here, :], up_mat, preferred_element_type=F32)
            act = exact_gelu(pre_act).astype(BF16)
            for piece in range(8):
                down_mat = jnp.concatenate(
                    [
                        jnp.concatenate([weights[c, t, piece // 2, piece % 2, 2 + i] for i in (0, 1)], axis=1)
                        for t in (0, 1)
                    ],
                    axis=0,
                )
                acc[here, piece * rows : (piece + 1) * rows] += jnp.dot(act, down_mat, preferred_element_type=F32)

        def drain(c):
            for i in range(len(SENDS)):
                message(c, i).wait_send()
            for dz in (0, 1):
                pair_message(c, dz, core).wait_send()

        def step(i, carry):
            def during(lag):
                return pl.when((i >= lag) & (i < n_chunks + lag))

            @during(0)
            def _():
                add_own(i)
                send_all(i, 0, 3)

            @during(3)
            def _():
                c = i - 3
                arrived(c, DX | DY, UPPER)
                arrived(c, DX | DY, LOWER)
                arrived(c, DX | DZ, WHOLE)
                arrived(c, DY | DZ, WHOLE)
                message(c, 7).start()
                early = c < EARLY

                @pl.when(early & (c % 2 == 1))
                def _():
                    message(c, 8, HOP3_X).start()

                @pl.when(early & (c % 2 == 0))
                def _():
                    message(c, 8, HOP3_Y).start()

                @pl.when(c >= EARLY)
                def _():
                    message(c, 8).start()

            @during(1)
            def _():
                arrived(i - 1, DZ, WHOLE)
                send_all(i - 1, 3, 5)

            @during(3)
            def _():
                pair_message(i - 3, 0, core).start()

            @during(LAST)
            def _():
                for dz in (0, 1):
                    pair_message(i - LAST, dz, 1 - core).wait_recv()
                multiply(i - LAST, 0)

            @during(1)
            def _():
                arrived(i - 1, DX, WHOLE)
                arrived(i - 1, DY, WHOLE)
                send_all(i - 1, 5, 7)

            @during(4)
            def _():
                arrived(i - 4, DX | DY | DZ, UPPER)
                arrived(i - 4, DX | DY | DZ, LOWER)
                pair_message(i - 4, 1, core).start()

            @during(LAST)
            def _():
                multiply(i - LAST, 1)

            @pl.when((i >= WINDOW - 1) & (i < n_chunks + WINDOW - 1))
            def _():
                drain(i - (WINDOW - 1))

            return carry

        lax.fori_loop(0, n_chunks + LAST, step, 0)
        for c in range(n_chunks + LAST - (WINDOW - 1), n_chunks):
            drain(c)


def last_kernel(learn_rate, w_up, w_down, g_up, g_down, acc, up_out, down_out, y_ref, result, zeros, sem, zero_sem):
    tokens = result.shape[0]
    is_gen = lax.axis_index("side") >= 2
    blocks = tokens // FINISH

    def zero_copies():
        for ref in (up_out.at[0, 0], down_out.at[0, 0]):
            high, wide = ref.shape
            for i in range(high // zeros.shape[0]):
                for j in range(wide // zeros.shape[1]):
                    part = ref.at[pl.ds(i * zeros.shape[0], zeros.shape[0]), pl.ds(j * zeros.shape[1], zeros.shape[1])]
                    yield pltpu.make_async_copy(zeros, part, zero_sem)

    @pl.when(is_gen)
    def _():
        zeros[...] = jnp.zeros_like(zeros)
        for copy in zero_copies():
            copy.start()

    def out(m):
        here = pl.ds(pl.multiple_of(m * FINISH, FINISH), FINISH)
        return pltpu.make_async_copy(result.at[here, :], y_ref.at[0, 0, here, :], sem)

    def finish(m, carry):
        here = pl.ds(pl.multiple_of(m * FINISH, FINISH), FINISH)
        result[here, :] = acc[here, :].astype(BF16)
        out(m).start()
        return carry

    lax.fori_loop(0, blocks, finish, 0)

    @pl.when(is_gen)
    def _():
        for copy in zero_copies():
            copy.wait()

    @pl.when(jnp.logical_not(is_gen))
    def _():
        rate = learn_rate[0]

        def body(w, g, new):
            new[...] = w[...] - rate * g[...]

        for w, g, new in ((w_up, g_up, up_out), (w_down, g_down, down_out)):
            high, wide = w.shape[2:]
            spec = pl.BlockSpec((high // 8, wide), lambda i: (i, 0))
            pltpu.emit_pipeline(body, grid=(8,), in_specs=[spec, spec], out_specs=[spec])(
                w.at[0, 0], g.at[0, 0], new.at[0, 0]
            )

    for m in range(blocks):
        out(m).wait()


def solution(mesh):
    up_spec = P("side", None, "rep", None)
    down_spec = P("side", None, None, "rep")
    copy_spec = P("side", "rep", None, None, None)
    token_spec = P("side", "rep", None, None)

    def local_step(w_up, w_down, g_up, g_down, learn_rate, old_up, old_down, prompts):
        n_chunks = w_up.shape[3] // LANES
        tokens, model = prompts.shape[2:]
        rows = w_up.shape[2]
        anywhere = pl.BlockSpec(memory_space=pl.ANY)
        scalar = pl.BlockSpec(memory_space=pltpu.SMEM)
        on_chip = pl.BlockSpec(memory_space=pltpu.VMEM)
        new_shapes = [jax.ShapeDtypeStruct(w.shape, F32) for w in (w_up, w_down)]
        total = pl.pallas_call(
            functools.partial(sync_kernel, n_chunks),
            out_shape=pltpu.VMEM((tokens, model), F32),
            in_specs=[scalar] + [anywhere] * 7,
            out_specs=on_chip,
            scratch_shapes=[
                pltpu.VMEM((n_chunks, 2, 4, 2, 4, LANES, LANES), BF16),
                pltpu.VMEM((tokens, model), BF16),
                pltpu.VMEM((2, 4, LANES, LANES), BF16),
                pltpu.VMEM((2, 2, rows, LANES), F32),
                pltpu.VMEM((2, 2, LANES, rows), F32),
                pltpu.SemaphoreType.DMA((n_chunks,)),
                pltpu.SemaphoreType.DMA((WINDOW, N_SEMS)),
                pltpu.SemaphoreType.DMA((n_chunks, len(ARRIVALS))),
                pltpu.SemaphoreType.DMA((n_chunks, 2)),
                pltpu.SemaphoreType.DMA((2, 4)),
                pltpu.SemaphoreType.DMA((2, 4)),
                pltpu.SemaphoreType.DMA,
                pltpu.SemaphoreType.REGULAR,
                pltpu.SemaphoreType.REGULAR,
            ],
            compiler_params=pltpu.CompilerParams(
                collective_id=0, has_side_effects=True, vmem_limit_bytes=VMEM_BYTES
            ),
        )(learn_rate, w_up, w_down, g_up, g_down, old_up, old_down, prompts)
        return pl.pallas_call(
            last_kernel,
            out_shape=new_shapes + [jax.ShapeDtypeStruct(prompts.shape, BF16)],
            in_specs=[scalar] + [anywhere] * 4 + [on_chip],
            out_specs=[anywhere] * 3,
            scratch_shapes=[
                pltpu.VMEM((tokens, model), BF16),
                pltpu.VMEM((256, 256), F32),
                pltpu.SemaphoreType.DMA,
                pltpu.SemaphoreType.DMA,
            ],
            compiler_params=pltpu.CompilerParams(vmem_limit_bytes=VMEM_BYTES),
        )(learn_rate, w_up, w_down, g_up, g_down, pltpu.with_memory_space_constraint(total, pltpu.VMEM))

    return jax.shard_map(
        local_step,
        mesh=mesh,
        in_specs=(up_spec, down_spec, up_spec, down_spec, P(None), copy_spec, copy_spec, token_spec),
        out_specs=(up_spec, down_spec, token_spec),
        check_vma=False,
    )
```

```python
import functools

import jax
import jax.numpy as jnp
from jax import lax
from jax.experimental import pallas as pl
from jax.experimental.pallas import tpu as pltpu
from jax.sharding import PartitionSpec as P

MESH = pl.DeviceIdType.MESH
F32 = jnp.float32
BF16 = jnp.bfloat16
LANES = 128
DX, DY, DZ = 1, 2, 4
WHOLE, UPPER, LOWER = (0, 2), (0, 1), (1, 2)
ARRIVALS = {
    (DX, WHOLE): 0, (DY, WHOLE): 1, (DZ, WHOLE): 2, (DX | DZ, WHOLE): 3, (DY | DZ, WHOLE): 4,
    (DX | DY, UPPER): 5, (DX | DY, LOWER): 6, (DX | DY | DZ, UPPER): 7, (DX | DY | DZ, LOWER): 8,
}
HOP1 = ((0, DX, WHOLE), (0, DY, WHOLE), (0, DZ, WHOLE))
HOP2 = ((DZ, DX, WHOLE), (DZ, DY, WHOLE), (DY, DX, UPPER), (DX, DY, LOWER))
HOP3 = ((DX | DY, DZ, UPPER), (DX | DY, DZ, LOWER))
HOP3_X, HOP3_Y = (DY | DZ, DX, LOWER), (DX | DZ, DY, LOWER)
SENDS = HOP1 + HOP2 + HOP3
N_SEMS = len(SENDS) + 2
WINDOW = 10
PACE = 3
EARLY = 28
LAST = 9
VMEM_BYTES = 54 * 2**20
FINISH = 64


def exact_gelu(v):
    return (0.5 * v) * (1.0 + lax.erf(v * (0.5**0.5)))


def sync_kernel(
    n_chunks, learn_rate, w_up, w_down, g_up, g_down, old_up, old_down, prompts, acc,
    weights, hidden, stale, up_pair, down_pair,
    own_recv, send_sem, recv_sem, pair_recv, stale_sem, fetch_sem, io_sem, pace_sem, credit_sem,
):
    side = lax.axis_index("side")
    rep = lax.axis_index("rep")
    core = rep % 2
    xpos = (rep // 2) % 2
    ypos = rep // 4
    rank = side % 2
    tokens = hidden.shape[0]
    rows = 2 * LANES
    n_parts = 2 * n_chunks

    barrier = pltpu.get_barrier_semaphore()

    def ping(sem, to_side, to_rep):
        pl.semaphore_signal(sem, inc=1, device_id=(to_side, to_rep), device_id_type=MESH)

    x_rep = rep + 2 * (1 - 2 * xpos)
    y_rep = rep + 4 * (1 - 2 * ypos)
    pair_rep = rep + (1 - 2 * core)
    z_side = 5 - side

    def columns(c):
        return pl.ds(pl.multiple_of(c * LANES, LANES), LANES)

    def prompts_in():
        return pltpu.make_async_copy(prompts.at[0, 0], hidden, io_sem)

    def residual(i, carry):
        here = pl.ds(pl.multiple_of(i * 64, 64), 64)
        acc[here, :] = hidden[here, :].astype(F32)
        return carry

    @pl.when(side < 2)
    def _():
        def fetches(c):
            slot = c % 2
            return [
                pltpu.make_async_copy(src, dst, fetch_sem.at[slot, i])
                for i, (src, dst) in enumerate(
                    (
                        (w_up.at[0, 0, :, columns(c)], up_pair.at[slot, 0]),
                        (g_up.at[0, 0, :, columns(c)], up_pair.at[slot, 1]),
                        (w_down.at[0, 0, columns(c), :], down_pair.at[slot, 0]),
                        (g_down.at[0, 0, columns(c), :], down_pair.at[slot, 1]),
                    )
                )
            ]

        def fetch(c):
            for copy in fetches(c):
                copy.start()

        def prepare(c):
            for copy in fetches(c):
                copy.wait()
            rate = learn_rate[0]
            slot = weights.at[c, rank, rep // 2, core]
            for i in (0, 1):
                part = slice(i * LANES, (i + 1) * LANES)
                for j, pair, here in ((0, up_pair, (part, slice(None))), (2, down_pair, (slice(None), part))):
                    old = pair[(c % 2, 0) + here]
                    slot[j + i] = ((old - rate * pair[(c % 2, 1) + here]) - old).astype(BF16)

        def delta_copy(s):
            ref = weights.at[s // 2, rank, rep // 2, core, pl.ds(2 * (s % 2), 2)]
            return pltpu.make_async_remote_copy(
                src_ref=ref, dst_ref=ref, send_sem=send_sem.at[s % WINDOW, 0], recv_sem=own_recv.at[s],
                device_id=(side + 2, rep), device_id_type=MESH,
            )

        fetch(0)
        fetch(1)
        prompts_in().start()
        ping(barrier, side + 2, rep)
        ping(barrier, 1 - side, rep)
        prepare(0)
        pl.semaphore_wait(barrier, 2)

        def send(s, carry):
            @pl.when(s >= PACE)
            def _():
                pl.semaphore_wait(credit_sem, 1)

            @pl.when((side == 0) & (s >= 1))
            def _():
                pl.semaphore_wait(pace_sem, 1)

            delta_copy(s).start()

            @pl.when((s % 2 == 0) & (s // 2 + 2 < n_chunks))
            def _():
                fetch(s // 2 + 2)

            @pl.when((s % 2 == 0) & (s // 2 + 1 < n_chunks))
            def _():
                prepare(s // 2 + 1)

            @pl.when(s >= 1)
            def _():
                delta_copy(s - 1).wait_send()

            @pl.when((side == 1) & (s >= 1))
            def _():
                ping(pace_sem, 0, rep)

            return carry

        lax.fori_loop(0, n_parts, send, 0)
        delta_copy(n_parts - 1).wait_send()
        prompts_in().wait()
        lax.fori_loop(0, tokens // 64, residual, 0)

    @pl.when(side >= 2)
    def _():
        prompts_in().start()

        def place(d):
            t = 1 - rank if d & DZ else rank
            yy = 1 - ypos if d & DY else ypos
            xx = 1 - xpos if d & DX else xpos
            return t, yy * 2 + xx

        def stale_copies(c):
            slot = stale.at[c % 2]
            first = pl.multiple_of(rep * rows, rows)

            def part(i):
                return pl.ds(first + i * LANES, LANES)

            return [
                pltpu.make_async_copy(old_up.at[0, 0, 0, part(i), columns(c)], slot.at[i], stale_sem.at[c % 2, i])
                for i in (0, 1)
            ] + [
                pltpu.make_async_copy(
                    old_down.at[0, 0, 0, columns(c), part(i)], slot.at[2 + i], stale_sem.at[c % 2, 2 + i]
                )
                for i in (0, 1)
            ]

        def blocks_of(c, d, blocks):
            t, yx = place(d)
            return weights.at[c // 2, t, yx, core, pl.ds(2 * (c % 2) + blocks[0], blocks[1] - blocks[0])]

        def message(c, i, route=None):
            d, axis, blocks = route or SENDS[i]
            ref = blocks_of(c, d, blocks)
            to = {DX: (side, x_rep), DY: (side, y_rep), DZ: (z_side, rep)}[axis]
            return pltpu.make_async_remote_copy(
                src_ref=ref, dst_ref=ref, send_sem=send_sem.at[c % WINDOW, i],
                recv_sem=recv_sem.at[c, ARRIVALS[d | axis, blocks]], device_id=to, device_id_type=MESH,
            )

        def arrived(c, d, blocks):
            ref = blocks_of(c, d, blocks)
            pltpu.make_async_remote_copy(
                src_ref=ref, dst_ref=ref, send_sem=send_sem.at[0, 0], recv_sem=recv_sem.at[c, ARRIVALS[d, blocks]],
                device_id=(side, rep), device_id_type=MESH,
            ).wait_recv()

        def pair_message(c, dz, of_core):
            t = 1 - rank if dz else rank
            ref = weights.at[c // 2, t, :, of_core, pl.ds(2 * (c % 2), 2)]
            return pltpu.make_async_remote_copy(
                src_ref=ref, dst_ref=ref, send_sem=send_sem.at[c % WINDOW, len(SENDS) + dz],
                recv_sem=pair_recv.at[c, dz], device_id=(side, pair_rep), device_id_type=MESH,
            )

        for c in (0, 1):
            for copy in stale_copies(c):
                copy.start()
        ping(barrier, side, x_rep)
        ping(barrier, side, y_rep)
        ping(barrier, side, pair_rep)
        ping(barrier, z_side, rep)
        ping(barrier, side - 2, rep)

        prompts_in().wait()
        lax.fori_loop(0, tokens // 64, residual, 0)
        pl.semaphore_wait(barrier, 5)

        def send_all(c, first, last):
            for i in range(first, last):
                message(c, i).start()

        def add_own(s):
            c, h = s // 2, s % 2
            slot = weights.at[c, rank, rep // 2, core]
            part = slot.at[pl.ds(2 * h, 2)]
            pltpu.make_async_remote_copy(
                src_ref=part, dst_ref=part, send_sem=send_sem.at[0, 0], recv_sem=own_recv.at[s],
                device_id=(side - 2, rep), device_id_type=MESH,
            ).wait_recv()

            @pl.when(h == 0)
            def _():
                for copy in stale_copies(c):
                    copy.wait()

            for i in (0, 1):
                new = stale[c % 2, 2 * h + i].astype(F32) + slot[2 * h + i].astype(F32)
                slot[2 * h + i] = new.astype(BF16)

            @pl.when(s + PACE < n_parts)
            def _():
                ping(credit_sem, side - 2, rep)

            @pl.when((h == 1) & (c + 2 < n_chunks))
            def _():
                for copy in stale_copies(c + 2):
                    copy.start()

        half = tokens // 2

        def multiply(c, m):
            here = pl.ds(pl.multiple_of(m * half, half), half)
            up_mat = jnp.concatenate(
                [weights[c, t, :, :, 0:2].reshape(acc.shape[1], LANES) for t in (0, 1)], axis=1
            )
            pre_act = jnp.dot(hidden[here, :], up_mat, preferred_element_type=F32)
            act = exact_gelu(pre_act).astype(BF16)
            for piece in range(8):
                down_mat = jnp.concatenate(
                    [
                        jnp.concatenate([weights[c, t, piece // 2, piece % 2, 2 + i] for i in (0, 1)], axis=1)
                        for t in (0, 1)
                    ],
                    axis=0,
                )
                acc[here, piece * rows : (piece + 1) * rows] += jnp.dot(act, down_mat, preferred_element_type=F32)

        def drain(c):
            for i in range(len(SENDS)):
                message(c, i).wait_send()
            for dz in (0, 1):
                pair_message(c, dz, core).wait_send()

        def step(i, carry):
            def during(lag):
                return pl.when((i >= lag) & (i < n_parts + lag))

            @during(LAST)
            def _():
                s = i - LAST

                @pl.when(s % 2 == 0)
                def _():
                    for part in (0, 1):
                        for dz in (0, 1):
                            pair_message(s + part, dz, 1 - core).wait_recv()

                multiply(s // 2, s % 2)

            @during(2)
            def _():
                arrived(i - 2, DX, WHOLE)
                arrived(i - 2, DY, WHOLE)
                send_all(i - 2, 5, 7)

            @during(0)
            def _():
                add_own(i)
                send_all(i, 0, 3)

            @during(2)
            def _():
                arrived(i - 2, DZ, WHOLE)
                send_all(i - 2, 3, 5)

            @during(4)
            def _():
                s = i - 4
                arrived(s, DX | DY, UPPER)
                arrived(s, DX | DY, LOWER)
                arrived(s, DX | DZ, WHOLE)
                arrived(s, DY | DZ, WHOLE)
                message(s, 7).start()
                early = s < EARLY
                odd = s // 2 % 2 == 1

                @pl.when(early & odd)
                def _():
                    message(s, 8, HOP3_X).start()

                @pl.when(early & jnp.logical_not(odd))
                def _():
                    message(s, 8, HOP3_Y).start()

                @pl.when(s >= EARLY)
                def _():
                    message(s, 8).start()

                pair_message(s, 0, core).start()

            @during(6)
            def _():
                arrived(i - 6, DX | DY | DZ, UPPER)
                arrived(i - 6, DX | DY | DZ, LOWER)
                pair_message(i - 6, 1, core).start()

            @during(WINDOW - 1)
            def _():
                drain(i - (WINDOW - 1))

            return carry

        lax.fori_loop(0, n_parts + LAST, step, 0)


def last_kernel(learn_rate, w_up, w_down, g_up, g_down, acc, up_out, down_out, y_ref, result, zeros, sem, zero_sem):
    tokens = result.shape[0]
    is_gen = lax.axis_index("side") >= 2
    blocks = tokens // FINISH

    def zero_copies():
        for ref in (up_out.at[0, 0], down_out.at[0, 0]):
            high, wide = ref.shape
            for i in range(high // zeros.shape[0]):
                for j in range(wide // zeros.shape[1]):
                    part = ref.at[pl.ds(i * zeros.shape[0], zeros.shape[0]), pl.ds(j * zeros.shape[1], zeros.shape[1])]
                    yield pltpu.make_async_copy(zeros, part, zero_sem)

    @pl.when(is_gen)
    def _():
        zeros[...] = jnp.zeros_like(zeros)
        for copy in zero_copies():
            copy.start()

    def out(m):
        here = pl.ds(pl.multiple_of(m * FINISH, FINISH), FINISH)
        return pltpu.make_async_copy(result.at[here, :], y_ref.at[0, 0, here, :], sem)

    def finish(m, carry):
        here = pl.ds(pl.multiple_of(m * FINISH, FINISH), FINISH)
        result[here, :] = acc[here, :].astype(BF16)
        out(m).start()
        return carry

    lax.fori_loop(0, blocks, finish, 0)

    @pl.when(is_gen)
    def _():
        for copy in zero_copies():
            copy.wait()

    @pl.when(jnp.logical_not(is_gen))
    def _():
        rate = learn_rate[0]

        def body(w, g, new):
            new[...] = w[...] - rate * g[...]

        for w, g, new in ((w_up, g_up, up_out), (w_down, g_down, down_out)):
            high, wide = w.shape[2:]
            spec = pl.BlockSpec((high // 8, wide), lambda i: (i, 0))
            pltpu.emit_pipeline(body, grid=(8,), in_specs=[spec, spec], out_specs=[spec])(
                w.at[0, 0], g.at[0, 0], new.at[0, 0]
            )

    for m in range(blocks):
        out(m).wait()


def solution(mesh):
    up_spec = P("side", None, "rep", None)
    down_spec = P("side", None, None, "rep")
    copy_spec = P("side", "rep", None, None, None)
    token_spec = P("side", "rep", None, None)

    def local_step(w_up, w_down, g_up, g_down, learn_rate, old_up, old_down, prompts):
        n_chunks = w_up.shape[3] // LANES
        tokens, model = prompts.shape[2:]
        rows = w_up.shape[2]
        anywhere = pl.BlockSpec(memory_space=pl.ANY)
        scalar = pl.BlockSpec(memory_space=pltpu.SMEM)
        on_chip = pl.BlockSpec(memory_space=pltpu.VMEM)
        new_shapes = [jax.ShapeDtypeStruct(w.shape, F32) for w in (w_up, w_down)]
        total = pl.pallas_call(
            functools.partial(sync_kernel, n_chunks),
            out_shape=pltpu.VMEM((tokens, model), F32),
            in_specs=[scalar] + [anywhere] * 7,
            out_specs=on_chip,
            scratch_shapes=[
                pltpu.VMEM((n_chunks, 2, 4, 2, 4, LANES, LANES), BF16),
                pltpu.VMEM((tokens, model), BF16),
                pltpu.VMEM((2, 4, LANES, LANES), BF16),
                pltpu.VMEM((2, 2, rows, LANES), F32),
                pltpu.VMEM((2, 2, LANES, rows), F32),
                pltpu.SemaphoreType.DMA((2 * n_chunks,)),
                pltpu.SemaphoreType.DMA((WINDOW, N_SEMS)),
                pltpu.SemaphoreType.DMA((2 * n_chunks, len(ARRIVALS))),
                pltpu.SemaphoreType.DMA((2 * n_chunks, 2)),
                pltpu.SemaphoreType.DMA((2, 4)),
                pltpu.SemaphoreType.DMA((2, 4)),
                pltpu.SemaphoreType.DMA,
                pltpu.SemaphoreType.REGULAR,
                pltpu.SemaphoreType.REGULAR,
            ],
            compiler_params=pltpu.CompilerParams(
                collective_id=0, has_side_effects=True, vmem_limit_bytes=VMEM_BYTES
            ),
        )(learn_rate, w_up, w_down, g_up, g_down, old_up, old_down, prompts)
        return pl.pallas_call(
            last_kernel,
            out_shape=new_shapes + [jax.ShapeDtypeStruct(prompts.shape, BF16)],
            in_specs=[scalar] + [anywhere] * 4 + [on_chip],
            out_specs=[anywhere] * 3,
            scratch_shapes=[
                pltpu.VMEM((tokens, model), BF16),
                pltpu.VMEM((256, 256), F32),
                pltpu.SemaphoreType.DMA,
                pltpu.SemaphoreType.DMA,
            ],
            compiler_params=pltpu.CompilerParams(vmem_limit_bytes=VMEM_BYTES),
        )(learn_rate, w_up, w_down, g_up, g_down, pltpu.with_memory_space_constraint(total, pltpu.VMEM))

    return jax.shard_map(
        local_step,
        mesh=mesh,
        in_specs=(up_spec, down_spec, up_spec, down_spec, P(None), copy_spec, copy_spec, token_spec),
        out_specs=(up_spec, down_spec, token_spec),
        check_vma=False,
    )
```

```python
import functools

import jax
import jax.numpy as jnp
from jax import lax
from jax.experimental import pallas as pl
from jax.experimental.pallas import tpu as pltpu
from jax.sharding import PartitionSpec as P

MESH = pl.DeviceIdType.MESH
F32 = jnp.float32
BF16 = jnp.bfloat16
LANES = 128
DX, DY, DZ = 1, 2, 4
WHOLE, UPPER, LOWER = (0, 2), (0, 1), (1, 2)
ARRIVALS = {
    (DX, WHOLE): 0, (DY, WHOLE): 1, (DZ, WHOLE): 2, (DX | DZ, WHOLE): 3, (DY | DZ, WHOLE): 4,
    (DX | DY, UPPER): 5, (DX | DY, LOWER): 6, (DX | DY | DZ, UPPER): 7, (DX | DY | DZ, LOWER): 8,
}
HOP1 = ((0, DX, WHOLE), (0, DY, WHOLE), (0, DZ, WHOLE))
HOP2 = ((DZ, DX, WHOLE), (DZ, DY, WHOLE), (DY, DX, UPPER), (DX, DY, LOWER))
HOP3 = ((DX | DY, DZ, UPPER), (DX | DY, DZ, LOWER))
HOP3_X, HOP3_Y = (DY | DZ, DX, LOWER), (DX | DZ, DY, LOWER)
SENDS = HOP1 + HOP2 + HOP3
N_SEMS = len(SENDS) + 2
WINDOW = 10
PACE = 4
EARLY = 26
LAST = 9
VMEM_BYTES = 54 * 2**20
FINISH = 64


def exact_gelu(v):
    return (0.5 * v) * (1.0 + lax.erf(v * (0.5**0.5)))


def sync_kernel(
    n_chunks, learn_rate, w_up, w_down, g_up, g_down, old_up, old_down, prompts, acc,
    weights, hidden, stale, up_pair, down_pair,
    own_recv, send_sem, recv_sem, pair_recv, stale_sem, fetch_sem, io_sem, pace_sem, credit_sem,
):
    side = lax.axis_index("side")
    rep = lax.axis_index("rep")
    core = rep % 2
    xpos = (rep // 2) % 2
    ypos = rep // 4
    rank = side % 2
    tokens = hidden.shape[0]
    rows = 2 * LANES
    n_parts = 2 * n_chunks

    barrier = pltpu.get_barrier_semaphore()

    def ping(sem, to_side, to_rep):
        pl.semaphore_signal(sem, inc=1, device_id=(to_side, to_rep), device_id_type=MESH)

    x_rep = rep + 2 * (1 - 2 * xpos)
    y_rep = rep + 4 * (1 - 2 * ypos)
    pair_rep = rep + (1 - 2 * core)
    z_side = 5 - side

    def columns(c):
        return pl.ds(pl.multiple_of(c * LANES, LANES), LANES)

    def prompts_in():
        return pltpu.make_async_copy(prompts.at[0, 0], hidden, io_sem)

    def residual(i, carry):
        here = pl.ds(pl.multiple_of(i * 64, 64), 64)
        acc[here, :] = hidden[here, :].astype(F32)
        return carry

    @pl.when(side < 2)
    def _():
        def fetches(c):
            slot = c % 2
            return [
                pltpu.make_async_copy(src, dst, fetch_sem.at[slot, i])
                for i, (src, dst) in enumerate(
                    (
                        (w_up.at[0, 0, :, columns(c)], up_pair.at[slot, 0]),
                        (g_up.at[0, 0, :, columns(c)], up_pair.at[slot, 1]),
                        (w_down.at[0, 0, columns(c), :], down_pair.at[slot, 0]),
                        (g_down.at[0, 0, columns(c), :], down_pair.at[slot, 1]),
                    )
                )
            ]

        def fetch(c):
            for copy in fetches(c):
                copy.start()

        def prepare(c):
            for copy in fetches(c):
                copy.wait()
            rate = learn_rate[0]
            slot = weights.at[c, rank, rep // 2, core]
            for i in (0, 1):
                part = slice(i * LANES, (i + 1) * LANES)
                for j, pair, here in ((0, up_pair, (part, slice(None))), (2, down_pair, (slice(None), part))):
                    old = pair[(c % 2, 0) + here]
                    slot[j + i] = ((old - rate * pair[(c % 2, 1) + here]) - old).astype(BF16)

        def delta_copy(s):
            ref = weights.at[s // 2, rank, rep // 2, core, pl.ds(2 * (s % 2), 2)]
            return pltpu.make_async_remote_copy(
                src_ref=ref, dst_ref=ref, send_sem=send_sem.at[s % WINDOW, 0], recv_sem=own_recv.at[s],
                device_id=(side + 2, rep), device_id_type=MESH,
            )

        fetch(0)
        fetch(1)
        prompts_in().start()
        ping(barrier, side + 2, rep)
        ping(barrier, 1 - side, rep)
        prepare(0)
        pl.semaphore_wait(barrier, 2)

        def send(s, carry):
            @pl.when(s >= PACE)
            def _():
                pl.semaphore_wait(credit_sem, 1)

            @pl.when((side == 0) & (s >= 2))
            def _():
                pl.semaphore_wait(pace_sem, 1)

            delta_copy(s).start()

            @pl.when((s % 2 == 0) & (s // 2 + 2 < n_chunks))
            def _():
                fetch(s // 2 + 2)

            @pl.when((s % 2 == 0) & (s // 2 + 1 < n_chunks))
            def _():
                prepare(s // 2 + 1)

            @pl.when(s >= 1)
            def _():
                delta_copy(s - 1).wait_send()

            @pl.when((side == 1) & (s >= 1) & (s < n_parts - 1))
            def _():
                ping(pace_sem, 0, rep)

            return carry

        lax.fori_loop(0, n_parts, send, 0)
        delta_copy(n_parts - 1).wait_send()
        prompts_in().wait()
        lax.fori_loop(0, tokens // 64, residual, 0)

    @pl.when(side >= 2)
    def _():
        prompts_in().start()

        def place(d):
            t = 1 - rank if d & DZ else rank
            yy = 1 - ypos if d & DY else ypos
            xx = 1 - xpos if d & DX else xpos
            return t, yy * 2 + xx

        def stale_copies(c):
            slot = stale.at[c % 2]
            first = pl.multiple_of(rep * rows, rows)

            def part(i):
                return pl.ds(first + i * LANES, LANES)

            return [
                pltpu.make_async_copy(old_up.at[0, 0, 0, part(i), columns(c)], slot.at[i], stale_sem.at[c % 2, i])
                for i in (0, 1)
            ] + [
                pltpu.make_async_copy(
                    old_down.at[0, 0, 0, columns(c), part(i)], slot.at[2 + i], stale_sem.at[c % 2, 2 + i]
                )
                for i in (0, 1)
            ]

        def blocks_of(c, d, blocks):
            t, yx = place(d)
            return weights.at[c // 2, t, yx, core, pl.ds(2 * (c % 2) + blocks[0], blocks[1] - blocks[0])]

        def message(c, i, route=None):
            d, axis, blocks = route or SENDS[i]
            ref = blocks_of(c, d, blocks)
            to = {DX: (side, x_rep), DY: (side, y_rep), DZ: (z_side, rep)}[axis]
            return pltpu.make_async_remote_copy(
                src_ref=ref, dst_ref=ref, send_sem=send_sem.at[c % WINDOW, i],
                recv_sem=recv_sem.at[c, ARRIVALS[d | axis, blocks]], device_id=to, device_id_type=MESH,
            )

        def arrived(c, d, blocks):
            ref = blocks_of(c, d, blocks)
            pltpu.make_async_remote_copy(
                src_ref=ref, dst_ref=ref, send_sem=send_sem.at[0, 0], recv_sem=recv_sem.at[c, ARRIVALS[d, blocks]],
                device_id=(side, rep), device_id_type=MESH,
            ).wait_recv()

        def pair_message(c, dz, of_core):
            t = 1 - rank if dz else rank
            ref = weights.at[c // 2, t, :, of_core, pl.ds(2 * (c % 2), 2)]
            return pltpu.make_async_remote_copy(
                src_ref=ref, dst_ref=ref, send_sem=send_sem.at[c % WINDOW, len(SENDS) + dz],
                recv_sem=pair_recv.at[c, dz], device_id=(side, pair_rep), device_id_type=MESH,
            )

        for c in (0, 1):
            for copy in stale_copies(c):
                copy.start()
        ping(barrier, side, x_rep)
        ping(barrier, side, y_rep)
        ping(barrier, side, pair_rep)
        ping(barrier, z_side, rep)
        ping(barrier, side - 2, rep)

        prompts_in().wait()
        lax.fori_loop(0, tokens // 64, residual, 0)
        pl.semaphore_wait(barrier, 5)

        def send_all(c, first, last):
            for i in range(first, last):
                message(c, i).start()

        def add_own(s):
            c, h = s // 2, s % 2
            slot = weights.at[c, rank, rep // 2, core]
            part = slot.at[pl.ds(2 * h, 2)]
            pltpu.make_async_remote_copy(
                src_ref=part, dst_ref=part, send_sem=send_sem.at[0, 0], recv_sem=own_recv.at[s],
                device_id=(side - 2, rep), device_id_type=MESH,
            ).wait_recv()

            @pl.when(h == 0)
            def _():
                for copy in stale_copies(c):
                    copy.wait()

            for i in (0, 1):
                new = stale[c % 2, 2 * h + i].astype(F32) + slot[2 * h + i].astype(F32)
                slot[2 * h + i] = new.astype(BF16)

            @pl.when(s + PACE < n_parts)
            def _():
                ping(credit_sem, side - 2, rep)

            @pl.when((h == 1) & (c + 2 < n_chunks))
            def _():
                for copy in stale_copies(c + 2):
                    copy.start()

        half = tokens // 2

        def multiply(c, m):
            here = pl.ds(pl.multiple_of(m * half, half), half)
            up_mat = jnp.concatenate(
                [weights[c, t, :, :, 0:2].reshape(acc.shape[1], LANES) for t in (0, 1)], axis=1
            )
            pre_act = jnp.dot(hidden[here, :], up_mat, preferred_element_type=F32)
            act = exact_gelu(pre_act).astype(BF16)
            for piece in range(8):
                down_mat = jnp.concatenate(
                    [
                        jnp.concatenate([weights[c, t, piece // 2, piece % 2, 2 + i] for i in (0, 1)], axis=1)
                        for t in (0, 1)
                    ],
                    axis=0,
                )
                acc[here, piece * rows : (piece + 1) * rows] += jnp.dot(act, down_mat, preferred_element_type=F32)

        def drain(c):
            for i in range(len(SENDS)):
                message(c, i).wait_send()
            for dz in (0, 1):
                pair_message(c, dz, core).wait_send()

        def step(i, carry):
            def during(lag):
                return pl.when((i >= lag) & (i < n_parts + lag))

            @during(LAST)
            def _():
                s = i - LAST

                @pl.when(s % 2 == 0)
                def _():
                    for part in (0, 1):
                        for dz in (0, 1):
                            pair_message(s + part, dz, 1 - core).wait_recv()

                multiply(s // 2, s % 2)

            @during(2)
            def _():
                arrived(i - 2, DX, WHOLE)
                arrived(i - 2, DY, WHOLE)
                send_all(i - 2, 5, 7)

            @during(0)
            def _():
                add_own(i)
                send_all(i, 0, 3)

            @during(2)
            def _():
                arrived(i - 2, DZ, WHOLE)
                send_all(i - 2, 3, 5)

            @during(4)
            def _():
                s = i - 4
                arrived(s, DX | DY, UPPER)
                arrived(s, DX | DY, LOWER)
                arrived(s, DX | DZ, WHOLE)
                arrived(s, DY | DZ, WHOLE)
                message(s, 7).start()
                early = s < EARLY
                odd = s // 2 % 2 == 1

                @pl.when(early & odd)
                def _():
                    message(s, 8, HOP3_X).start()

                @pl.when(early & jnp.logical_not(odd))
                def _():
                    message(s, 8, HOP3_Y).start()

                @pl.when(s >= EARLY)
                def _():
                    message(s, 8).start()

                pair_message(s, 0, core).start()

            @during(6)
            def _():
                arrived(i - 6, DX | DY | DZ, UPPER)
                arrived(i - 6, DX | DY | DZ, LOWER)
                pair_message(i - 6, 1, core).start()

            @during(WINDOW - 1)
            def _():
                drain(i - (WINDOW - 1))

            return carry

        lax.fori_loop(0, n_parts + LAST, step, 0)


def last_kernel(learn_rate, w_up, w_down, g_up, g_down, acc, up_out, down_out, y_ref, result, zeros, sem, zero_sem):
    tokens = result.shape[0]
    is_gen = lax.axis_index("side") >= 2
    blocks = tokens // FINISH

    def zero_copies():
        for ref in (up_out.at[0, 0], down_out.at[0, 0]):
            high, wide = ref.shape
            for i in range(high // zeros.shape[0]):
                for j in range(wide // zeros.shape[1]):
                    part = ref.at[pl.ds(i * zeros.shape[0], zeros.shape[0]), pl.ds(j * zeros.shape[1], zeros.shape[1])]
                    yield pltpu.make_async_copy(zeros, part, zero_sem)

    @pl.when(is_gen)
    def _():
        zeros[...] = jnp.zeros_like(zeros)
        for copy in zero_copies():
            copy.start()

    def out(m):
        here = pl.ds(pl.multiple_of(m * FINISH, FINISH), FINISH)
        return pltpu.make_async_copy(result.at[here, :], y_ref.at[0, 0, here, :], sem)

    def finish(m, carry):
        here = pl.ds(pl.multiple_of(m * FINISH, FINISH), FINISH)
        result[here, :] = acc[here, :].astype(BF16)
        out(m).start()
        return carry

    lax.fori_loop(0, blocks, finish, 0)

    @pl.when(is_gen)
    def _():
        for copy in zero_copies():
            copy.wait()

    @pl.when(jnp.logical_not(is_gen))
    def _():
        rate = learn_rate[0]

        def body(w, g, new):
            new[...] = w[...] - rate * g[...]

        for w, g, new in ((w_up, g_up, up_out), (w_down, g_down, down_out)):
            high, wide = w.shape[2:]
            spec = pl.BlockSpec((high // 8, wide), lambda i: (i, 0))
            pltpu.emit_pipeline(body, grid=(8,), in_specs=[spec, spec], out_specs=[spec])(
                w.at[0, 0], g.at[0, 0], new.at[0, 0]
            )

    for m in range(blocks):
        out(m).wait()


def solution(mesh):
    up_spec = P("side", None, "rep", None)
    down_spec = P("side", None, None, "rep")
    copy_spec = P("side", "rep", None, None, None)
    token_spec = P("side", "rep", None, None)

    def local_step(w_up, w_down, g_up, g_down, learn_rate, old_up, old_down, prompts):
        n_chunks = w_up.shape[3] // LANES
        tokens, model = prompts.shape[2:]
        rows = w_up.shape[2]
        anywhere = pl.BlockSpec(memory_space=pl.ANY)
        scalar = pl.BlockSpec(memory_space=pltpu.SMEM)
        on_chip = pl.BlockSpec(memory_space=pltpu.VMEM)
        new_shapes = [jax.ShapeDtypeStruct(w.shape, F32) for w in (w_up, w_down)]
        total = pl.pallas_call(
            functools.partial(sync_kernel, n_chunks),
            out_shape=pltpu.VMEM((tokens, model), F32),
            in_specs=[scalar] + [anywhere] * 7,
            out_specs=on_chip,
            scratch_shapes=[
                pltpu.VMEM((n_chunks, 2, 4, 2, 4, LANES, LANES), BF16),
                pltpu.VMEM((tokens, model), BF16),
                pltpu.VMEM((2, 4, LANES, LANES), BF16),
                pltpu.VMEM((2, 2, rows, LANES), F32),
                pltpu.VMEM((2, 2, LANES, rows), F32),
                pltpu.SemaphoreType.DMA((2 * n_chunks,)),
                pltpu.SemaphoreType.DMA((WINDOW, N_SEMS)),
                pltpu.SemaphoreType.DMA((2 * n_chunks, len(ARRIVALS))),
                pltpu.SemaphoreType.DMA((2 * n_chunks, 2)),
                pltpu.SemaphoreType.DMA((2, 4)),
                pltpu.SemaphoreType.DMA((2, 4)),
                pltpu.SemaphoreType.DMA,
                pltpu.SemaphoreType.REGULAR,
                pltpu.SemaphoreType.REGULAR,
            ],
            compiler_params=pltpu.CompilerParams(
                collective_id=0, has_side_effects=True, vmem_limit_bytes=VMEM_BYTES
            ),
        )(learn_rate, w_up, w_down, g_up, g_down, old_up, old_down, prompts)
        return pl.pallas_call(
            last_kernel,
            out_shape=new_shapes + [jax.ShapeDtypeStruct(prompts.shape, BF16)],
            in_specs=[scalar] + [anywhere] * 4 + [on_chip],
            out_specs=[anywhere] * 3,
            scratch_shapes=[
                pltpu.VMEM((tokens, model), BF16),
                pltpu.VMEM((256, 256), F32),
                pltpu.SemaphoreType.DMA,
                pltpu.SemaphoreType.DMA,
            ],
            compiler_params=pltpu.CompilerParams(vmem_limit_bytes=VMEM_BYTES),
        )(learn_rate, w_up, w_down, g_up, g_down, pltpu.with_memory_space_constraint(total, pltpu.VMEM))

    return jax.shard_map(
        local_step,
        mesh=mesh,
        in_specs=(up_spec, down_spec, up_spec, down_spec, P(None), copy_spec, copy_spec, token_spec),
        out_specs=(up_spec, down_spec, token_spec),
        check_vma=False,
    )
```

```python
import functools

import jax
import jax.numpy as jnp
from jax import lax
from jax.experimental import pallas as pl
from jax.experimental.pallas import tpu as pltpu
from jax.sharding import PartitionSpec as P

MESH = pl.DeviceIdType.MESH
F32 = jnp.float32
BF16 = jnp.bfloat16
LANES = 128
DX, DY, DZ = 1, 2, 4
WHOLE, UPPER, LOWER = (0, 4), (0, 2), (2, 4)
ARRIVALS = {
    (DX, WHOLE): 0, (DY, WHOLE): 1, (DZ, WHOLE): 2, (DX | DZ, WHOLE): 3, (DY | DZ, WHOLE): 4,
    (DX | DY, UPPER): 5, (DX | DY, LOWER): 6, (DX | DY | DZ, UPPER): 7, (DX | DY | DZ, LOWER): 8,
}
HOP1 = ((0, DX, WHOLE), (0, DY, WHOLE), (0, DZ, WHOLE))
HOP2 = ((DZ, DX, WHOLE), (DZ, DY, WHOLE), (DY, DX, UPPER), (DX, DY, LOWER))
HOP3 = ((DX | DY, DZ, UPPER), (DX | DY, DZ, LOWER))
HOP3_X, HOP3_Y = (DY | DZ, DX, LOWER), (DX | DZ, DY, LOWER)
SENDS = HOP1 + HOP2 + HOP3
N_SEMS = len(SENDS) + 2
WINDOW = 8
PACE = 2
EARLY = 10
LAST = 5
VMEM_BYTES = 54 * 2**20
FINISH = 64


def exact_gelu(v):
    return (0.5 * v) * (1.0 + lax.erf(v * (0.5**0.5)))


def sync_kernel(
    n_chunks, learn_rate, w_up, w_down, g_up, g_down, old_up, old_down, prompts, acc,
    weights, hidden, stale, up_pair, down_pair,
    own_recv, send_sem, recv_sem, pair_recv, stale_sem, fetch_sem, io_sem, pace_sem, credit_sem,
):
    side = lax.axis_index("side")
    rep = lax.axis_index("rep")
    core = rep % 2
    xpos = (rep // 2) % 2
    ypos = rep // 4
    rank = side % 2
    tokens = hidden.shape[0]
    rows = 2 * LANES

    barrier = pltpu.get_barrier_semaphore()

    def ping(sem, to_side, to_rep):
        pl.semaphore_signal(sem, inc=1, device_id=(to_side, to_rep), device_id_type=MESH)

    x_rep = rep + 2 * (1 - 2 * xpos)
    y_rep = rep + 4 * (1 - 2 * ypos)
    pair_rep = rep + (1 - 2 * core)
    z_side = 5 - side

    def columns(c):
        return pl.ds(pl.multiple_of(c * LANES, LANES), LANES)

    def prompts_in():
        return pltpu.make_async_copy(prompts.at[0, 0], hidden, io_sem)

    def residual(i, carry):
        here = pl.ds(pl.multiple_of(i * 64, 64), 64)
        acc[here, :] = hidden[here, :].astype(F32)
        return carry

    @pl.when(side < 2)
    def _():
        def fetches(c):
            slot = c % 2
            return [
                pltpu.make_async_copy(src, dst, fetch_sem.at[slot, i])
                for i, (src, dst) in enumerate(
                    (
                        (w_up.at[0, 0, :, columns(c)], up_pair.at[slot, 0]),
                        (g_up.at[0, 0, :, columns(c)], up_pair.at[slot, 1]),
                        (w_down.at[0, 0, columns(c), :], down_pair.at[slot, 0]),
                        (g_down.at[0, 0, columns(c), :], down_pair.at[slot, 1]),
                    )
                )
            ]

        def fetch(c):
            for copy in fetches(c):
                copy.start()

        def prepare(c):
            for copy in fetches(c):
                copy.wait()
            rate = learn_rate[0]
            slot = weights.at[c, rank, rep // 2, core]
            for i in (0, 1):
                part = slice(i * LANES, (i + 1) * LANES)
                for j, pair, here in ((0, up_pair, (part, slice(None))), (2, down_pair, (slice(None), part))):
                    old = pair[(c % 2, 0) + here]
                    slot[j + i] = ((old - rate * pair[(c % 2, 1) + here]) - old).astype(BF16)

        def delta_copy(c):
            ref = weights.at[c, rank, rep // 2, core]
            return pltpu.make_async_remote_copy(
                src_ref=ref, dst_ref=ref, send_sem=send_sem.at[c % WINDOW, 0], recv_sem=own_recv.at[c],
                device_id=(side + 2, rep), device_id_type=MESH,
            )

        fetch(0)
        fetch(1)
        prompts_in().start()
        ping(barrier, side + 2, rep)
        ping(barrier, 1 - side, rep)
        prepare(0)
        pl.semaphore_wait(barrier, 2)

        def send(c, carry):
            @pl.when(c >= PACE)
            def _():
                pl.semaphore_wait(credit_sem, 1)

            @pl.when((side == 0) & (c >= 1))
            def _():
                pl.semaphore_wait(pace_sem, 1)

            delta_copy(c).start()

            @pl.when(c + 2 < n_chunks)
            def _():
                fetch(c + 2)

            @pl.when(c + 1 < n_chunks)
            def _():
                prepare(c + 1)

            @pl.when(c >= 1)
            def _():
                delta_copy(c - 1).wait_send()

            @pl.when((side == 1) & (c >= 1))
            def _():
                ping(pace_sem, 0, rep)

            return carry

        lax.fori_loop(0, n_chunks, send, 0)
        delta_copy(n_chunks - 1).wait_send()
        prompts_in().wait()
        lax.fori_loop(0, tokens // 64, residual, 0)

    @pl.when(side >= 2)
    def _():
        prompts_in().start()

        def place(d):
            t = 1 - rank if d & DZ else rank
            yy = 1 - ypos if d & DY else ypos
            xx = 1 - xpos if d & DX else xpos
            return t, yy * 2 + xx

        def stale_copies(c):
            slot = stale.at[c % 2]
            first = pl.multiple_of(rep * rows, rows)

            def part(i):
                return pl.ds(first + i * LANES, LANES)

            return [
                pltpu.make_async_copy(old_up.at[0, 0, 0, part(i), columns(c)], slot.at[i], stale_sem.at[c % 2, i])
                for i in (0, 1)
            ] + [
                pltpu.make_async_copy(
                    old_down.at[0, 0, 0, columns(c), part(i)], slot.at[2 + i], stale_sem.at[c % 2, 2 + i]
                )
                for i in (0, 1)
            ]

        def blocks_of(c, d, blocks):
            t, yx = place(d)
            return weights.at[c, t, yx, core, pl.ds(blocks[0], blocks[1] - blocks[0])]

        def message(c, i, route=None):
            d, axis, blocks = route or SENDS[i]
            ref = blocks_of(c, d, blocks)
            to = {DX: (side, x_rep), DY: (side, y_rep), DZ: (z_side, rep)}[axis]
            return pltpu.make_async_remote_copy(
                src_ref=ref, dst_ref=ref, send_sem=send_sem.at[c % WINDOW, i],
                recv_sem=recv_sem.at[c, ARRIVALS[d | axis, blocks]], device_id=to, device_id_type=MESH,
            )

        def arrived(c, d, blocks):
            ref = blocks_of(c, d, blocks)
            pltpu.make_async_remote_copy(
                src_ref=ref, dst_ref=ref, send_sem=send_sem.at[0, 0], recv_sem=recv_sem.at[c, ARRIVALS[d, blocks]],
                device_id=(side, rep), device_id_type=MESH,
            ).wait_recv()

        def pair_message(c, dz, of_core):
            t = 1 - rank if dz else rank
            ref = weights.at[c, t, :, of_core]
            return pltpu.make_async_remote_copy(
                src_ref=ref, dst_ref=ref, send_sem=send_sem.at[c % WINDOW, len(SENDS) + dz],
                recv_sem=pair_recv.at[c, dz], device_id=(side, pair_rep), device_id_type=MESH,
            )

        for c in (0, 1):
            for copy in stale_copies(c):
                copy.start()
        ping(barrier, side, x_rep)
        ping(barrier, side, y_rep)
        ping(barrier, side, pair_rep)
        ping(barrier, z_side, rep)
        ping(barrier, side - 2, rep)

        prompts_in().wait()
        lax.fori_loop(0, tokens // 64, residual, 0)
        pl.semaphore_wait(barrier, 5)

        def send_all(c, first, last):
            for i in range(first, last):
                message(c, i).start()

        def add_own(c):
            slot = weights.at[c, rank, rep // 2, core]
            pltpu.make_async_remote_copy(
                src_ref=slot, dst_ref=slot, send_sem=send_sem.at[0, 0], recv_sem=own_recv.at[c],
                device_id=(side - 2, rep), device_id_type=MESH,
            ).wait_recv()
            for copy in stale_copies(c):
                copy.wait()
            for i in range(4):
                slot[i] = (stale[c % 2, i].astype(F32) + slot[i].astype(F32)).astype(BF16)

            @pl.when(c + PACE < n_chunks)
            def _():
                ping(credit_sem, side - 2, rep)

            @pl.when(c + 2 < n_chunks)
            def _():
                for copy in stale_copies(c + 2):
                    copy.start()

        half = tokens // 2

        def multiply(c, m):
            here = slice(m * half, (m + 1) * half)
            up_mat = jnp.concatenate(
                [weights[c, t, :, :, 0:2].reshape(acc.shape[1], LANES) for t in (0, 1)], axis=1
            )
            pre_act = jnp.dot(hidden[here, :], up_mat, preferred_element_type=F32)
            act = exact_gelu(pre_act).astype(BF16)
            for piece in range(8):
                down_mat = jnp.concatenate(
                    [
                        jnp.concatenate([weights[c, t, piece // 2, piece % 2, 2 + i] for i in (0, 1)], axis=1)
                        for t in (0, 1)
                    ],
                    axis=0,
                )
                acc[here, piece * rows : (piece + 1) * rows] += jnp.dot(act, down_mat, preferred_element_type=F32)

        def drain(c):
            for i in range(len(SENDS)):
                message(c, i).wait_send()
            for dz in (0, 1):
                pair_message(c, dz, core).wait_send()

        def step(i, carry):
            def during(lag):
                return pl.when((i >= lag) & (i < n_chunks + lag))

            @during(0)
            def _():
                add_own(i)
                send_all(i, 0, 3)

            @during(3)
            def _():
                c = i - 3
                arrived(c, DX | DY, UPPER)
                arrived(c, DX | DY, LOWER)
                arrived(c, DX | DZ, WHOLE)
                arrived(c, DY | DZ, WHOLE)
                message(c, 7).start()
                early = c < EARLY

                @pl.when(early & (c % 2 == 1))
                def _():
                    message(c, 8, HOP3_X).start()

                @pl.when(early & (c % 2 == 0))
                def _():
                    message(c, 8, HOP3_Y).start()

                @pl.when(c >= EARLY)
                def _():
                    message(c, 8).start()

            @during(1)
            def _():
                arrived(i - 1, DZ, WHOLE)
                send_all(i - 1, 3, 5)

            @during(3)
            def _():
                pair_message(i - 3, 0, core).start()

            @during(LAST)
            def _():
                for dz in (0, 1):
                    pair_message(i - LAST, dz, 1 - core).wait_recv()
                multiply(i - LAST, 0)

            @during(1)
            def _():
                arrived(i - 1, DX, WHOLE)
                arrived(i - 1, DY, WHOLE)
                send_all(i - 1, 5, 7)

            @during(4)
            def _():
                arrived(i - 4, DX | DY | DZ, UPPER)
                arrived(i - 4, DX | DY | DZ, LOWER)
                pair_message(i - 4, 1, core).start()

            @during(LAST)
            def _():
                multiply(i - LAST, 1)

            @pl.when((i >= WINDOW - 1) & (i < n_chunks + WINDOW - 1))
            def _():
                drain(i - (WINDOW - 1))

            return carry

        lax.fori_loop(0, n_chunks + LAST, step, 0)
        for c in range(n_chunks + LAST - (WINDOW - 1), n_chunks):
            drain(c)


def last_kernel(learn_rate, w_up, w_down, g_up, g_down, acc, up_out, down_out, y_ref, result, zeros, sem, zero_sem):
    tokens = result.shape[0]
    is_gen = lax.axis_index("side") >= 2
    blocks = tokens // FINISH

    def zero_copies():
        for ref in (up_out.at[0, 0], down_out.at[0, 0]):
            high, wide = ref.shape
            for i in range(high // zeros.shape[0]):
                for j in range(wide // zeros.shape[1]):
                    part = ref.at[pl.ds(i * zeros.shape[0], zeros.shape[0]), pl.ds(j * zeros.shape[1], zeros.shape[1])]
                    yield pltpu.make_async_copy(zeros, part, zero_sem)

    @pl.when(is_gen)
    def _():
        zeros[...] = jnp.zeros_like(zeros)
        for copy in zero_copies():
            copy.start()

    def out(m):
        here = pl.ds(pl.multiple_of(m * FINISH, FINISH), FINISH)
        return pltpu.make_async_copy(result.at[here, :], y_ref.at[0, 0, here, :], sem)

    def finish(m, carry):
        here = pl.ds(pl.multiple_of(m * FINISH, FINISH), FINISH)
        result[here, :] = acc[here, :].astype(BF16)
        out(m).start()
        return carry

    lax.fori_loop(0, blocks, finish, 0)

    @pl.when(is_gen)
    def _():
        for copy in zero_copies():
            copy.wait()

    @pl.when(jnp.logical_not(is_gen))
    def _():
        rate = learn_rate[0]

        def body(w, g, new):
            new[...] = w[...] - rate * g[...]

        for w, g, new in ((w_up, g_up, up_out), (w_down, g_down, down_out)):
            high, wide = w.shape[2:]
            spec = pl.BlockSpec((high // 8, wide), lambda i: (i, 0))
            pltpu.emit_pipeline(body, grid=(8,), in_specs=[spec, spec], out_specs=[spec])(
                w.at[0, 0], g.at[0, 0], new.at[0, 0]
            )

    for m in range(blocks):
        out(m).wait()


def solution(mesh):
    up_spec = P("side", None, "rep", None)
    down_spec = P("side", None, None, "rep")
    copy_spec = P("side", "rep", None, None, None)
    token_spec = P("side", "rep", None, None)

    def local_step(w_up, w_down, g_up, g_down, learn_rate, old_up, old_down, prompts):
        n_chunks = w_up.shape[3] // LANES
        tokens, model = prompts.shape[2:]
        rows = w_up.shape[2]
        anywhere = pl.BlockSpec(memory_space=pl.ANY)
        scalar = pl.BlockSpec(memory_space=pltpu.SMEM)
        on_chip = pl.BlockSpec(memory_space=pltpu.VMEM)
        new_shapes = [jax.ShapeDtypeStruct(w.shape, F32) for w in (w_up, w_down)]
        total = pl.pallas_call(
            functools.partial(sync_kernel, n_chunks),
            out_shape=pltpu.VMEM((tokens, model), F32),
            in_specs=[scalar] + [anywhere] * 7,
            out_specs=on_chip,
            scratch_shapes=[
                pltpu.VMEM((n_chunks, 2, 4, 2, 4, LANES, LANES), BF16),
                pltpu.VMEM((tokens, model), BF16),
                pltpu.VMEM((2, 4, LANES, LANES), BF16),
                pltpu.VMEM((2, 2, rows, LANES), F32),
                pltpu.VMEM((2, 2, LANES, rows), F32),
                pltpu.SemaphoreType.DMA((n_chunks,)),
                pltpu.SemaphoreType.DMA((WINDOW, N_SEMS)),
                pltpu.SemaphoreType.DMA((n_chunks, len(ARRIVALS))),
                pltpu.SemaphoreType.DMA((n_chunks, 2)),
                pltpu.SemaphoreType.DMA((2, 4)),
                pltpu.SemaphoreType.DMA((2, 4)),
                pltpu.SemaphoreType.DMA,
                pltpu.SemaphoreType.REGULAR,
                pltpu.SemaphoreType.REGULAR,
            ],
            compiler_params=pltpu.CompilerParams(
                collective_id=0, has_side_effects=True, vmem_limit_bytes=VMEM_BYTES
            ),
        )(learn_rate, w_up, w_down, g_up, g_down, old_up, old_down, prompts)
        return pl.pallas_call(
            last_kernel,
            out_shape=new_shapes + [jax.ShapeDtypeStruct(prompts.shape, BF16)],
            in_specs=[scalar] + [anywhere] * 4 + [on_chip],
            out_specs=[anywhere] * 3,
            scratch_shapes=[
                pltpu.VMEM((tokens, model), BF16),
                pltpu.VMEM((256, 256), F32),
                pltpu.SemaphoreType.DMA,
                pltpu.SemaphoreType.DMA,
            ],
            compiler_params=pltpu.CompilerParams(vmem_limit_bytes=VMEM_BYTES),
        )(learn_rate, w_up, w_down, g_up, g_down, pltpu.with_memory_space_constraint(total, pltpu.VMEM))

    return jax.shard_map(
        local_step,
        mesh=mesh,
        in_specs=(up_spec, down_spec, up_spec, down_spec, P(None), copy_spec, copy_spec, token_spec),
        out_specs=(up_spec, down_spec, token_spec),
        check_vma=False,
    )
```
